32 devices in a mesh: groups: 2 (over x), dom: 16 (over z, y, core).
Axes of the slice: x: 2, y: 2, z: 4, core: 2. Of those that a mesh axis runs over, the one named last changes fastest.
Arguments:
- node_latent: bfloat16 [32768, 128], P(('groups', 'dom')), parts along dimension 0, may hold values from -6 to 6
- edge_latent: bfloat16 [196608, 128], P(('groups', 'dom')), parts along dimension 0, may hold values from -6 to 6
- node_cot: bfloat16 [32768, 128], P(('groups', 'dom')), parts along dimension 0, may hold values from -6 to 6
- edge_cot: bfloat16 [196608, 128], P(('groups', 'dom')), parts along dimension 0, may hold values from -6 to 6
- base_pos: float32 [3, 32768], P(None, ('groups', 'dom')), parts along dimension 1
- centers: float32 [3, 2048], replicated, may hold values from 0 to 1
- amplitudes: float32 [3, 2048], replicated, may hold values from -0.3 to 0.3
- edge_in: bfloat16 [384, 128], replicated, may hold values from -0.3125 to 0.3125
- edge_geo: float32 [4, 128], replicated, may hold values from -3 to 3
- edge_out: bfloat16 [128, 128], replicated, may hold values from -0.5 to 0.5
- edge_gain: float32 [128], replicated, may hold values from 0.5 to 1.5
- node_in: bfloat16 [256, 128], replicated, may hold values from -0.375 to 0.375
- node_out: bfloat16 [128, 128], replicated, may hold values from -0.5 to 0.5
- node_gain: float32 [128], replicated, may hold values from 0.5 to 1.5
- senders: int32 [196608], P(('groups', 'dom')), parts along dimension 0, may hold values from 0 to 3071, as said below
- receivers: int32 [196608], P(('groups', 'dom')), parts along dimension 0, may hold values from 0 to 1023
- send_rows: int32 [32, 16, 128], P(('groups', 'dom')), parts along dimension 0, may hold values from 0 to 1023
Outputs:
- grad_nodes: float32 [32768, 128], P(('groups', 'dom')), parts along dimension 0
- grad_edges: float32 [196608, 128], P(('groups', 'dom')), parts along dimension 0
- grad_controls: float32 [6, 2048], P('groups'), parts along dimension 0
The draws below stay inside these ranges and needn't reach their ends.
There are 2 independent parts, one for each index of `groups`. The reference program is written for one: setup_inputs(seed, part) draws one part's arguments, and reference() takes and returns one part's arrays. A program takes and returns all parts, laid end to end along the dimension named above; an argument that names none is the same for every part. Nothing has to cross between parts.
Inputs may be any that keep to these rules, and one draw needn't show every extreme that they name: `senders`: for edge j in partition q = j // 6144: a value below 1024 is an own node; a value v of 1024 or more names slot (v - 1024) % 128 of the block from partition p = (v - 1024) // 128, and 1 <= |p - q| <= 2. Every partition has an edge using slot 127 of some block.
All inputs are finite; a program needn't handle non-finite values.
Results may differ from the reference program's by a relative error of at most 0.0085.
Values may be sent and summed in bfloat16 or wider, within the bound.
A program may use at most 128 MiB of HBM per device.

```python
import jax
import jax.numpy as jnp
from jax import lax

LATENT = 128
CTRL = 2048
NV_DEV = 1024
HALO = 128
REACH = 2
NE_DEV = 6144
NODES = 16384
EDGES = 98304
N_DOM = 16


def draw_base_pos(key, part):
    uniform_draw = jax.random.uniform(jax.random.fold_in(key, 3), (3, NODES), jnp.float32)
    owner = (jnp.arange(NODES, dtype=jnp.int32) // NV_DEV).astype(jnp.float32)
    across = (owner + uniform_draw[0]) / N_DOM
    second = uniform_draw[1]
    third = uniform_draw[2]
    return jnp.stack([across, second, third], axis=0).astype(jnp.float32)


def draw_senders(key, part):
    keys = jax.random.split(jax.random.fold_in(key, 11), 6)
    edge_ids = jnp.arange(EDGES, dtype=jnp.int32)
    owner = edge_ids // NE_DEV
    within = edge_ids % NE_DEV
    local_pick = jax.random.randint(keys[0], (EDGES,), 0, NV_DEV, dtype=jnp.int32)
    share = jax.random.randint(keys[1], (N_DOM,), 10, 50, dtype=jnp.int32)
    dice = jax.random.randint(keys[2], (EDGES,), 0, 100, dtype=jnp.int32)
    first = within == 0
    choose = jnp.where(first, 0, jax.random.randint(keys[3], (EDGES,), 0, 2 * REACH, dtype=jnp.int32))
    offset_val = jnp.where(choose < REACH, choose - REACH, choose - REACH + 1)
    source = owner + offset_val
    source = jnp.where((source >= 0) & (source < N_DOM), source, owner - offset_val)
    capacity = jax.random.randint(keys[4], (N_DOM, 2 * REACH), HALO // 4, HALO + 1, dtype=jnp.int32)
    limit = jnp.where(choose == 0, HALO, capacity[owner, choose])
    slot_pick = jax.random.randint(keys[5], (EDGES,), 0, 1 << 20, dtype=jnp.int32) % limit
    slot_pick = jnp.where(first, HALO - 1, slot_pick)
    remote = (dice < share[owner]) | first
    return jnp.where(remote, NV_DEV + source * HALO + slot_pick, local_pick).astype(jnp.int32)


def place_ends(array, stream_key, low, top_value):
    index_at = [jax.random.randint(jax.random.fold_in(stream_key, axis), (), 0, length) for axis, length in enumerate(array.shape)]
    widest = array.shape.index(max(array.shape))
    next_to = index_at[:widest] + [(index_at[widest] + 1) % array.shape[widest]] + index_at[widest + 1:]
    return array.at[tuple(index_at)].set(low).at[tuple(next_to)].set(top_value)


def block_levels(key, shape, cuts, smallest, largest):
    level = 1.0
    for axis_at, shards_of in cuts:
        draws = jax.random.uniform(jax.random.fold_in(jax.random.fold_in(key, 6), axis_at), (shards_of,), jnp.float32, smallest / len(cuts), largest / len(cuts))
        level = level * jnp.repeat(jnp.exp(draws), shape[axis_at] // shards_of).reshape((-1,) + (1,) * (len(shape) - 1 - axis_at))
    return level


def normal_values(key, dims, scale, most, cuts=(), held_as=jnp.bfloat16):
    result = jax.random.normal(key, dims, jnp.float32) * scale
    if len(cuts) > 0:
        result = block_levels(key, dims, cuts, -0.22, 0.18) * result
    return jnp.clip(result, min=-most, max=most).astype(held_as)


def setup_inputs(seed: int = 0, part: int = 0) -> dict:
    key_of = jax.random.split(jax.random.key(seed), 18)
    own_keys = jax.random.split(jax.random.fold_in(key_of[17], part), 18)
    node_latent = normal_values(own_keys[0], (NODES, LATENT), 1.0, 6.0, ((0, 16),))
    edge_latent = normal_values(own_keys[1], (EDGES, LATENT), 1.0, 6.0, ((0, 16),))
    node_cot = normal_values(own_keys[2], (NODES, LATENT), 1.0, 6.0, ((0, 16),))
    edge_cot = normal_values(own_keys[3], (EDGES, LATENT), 1.0, 6.0, ((0, 16),))
    base_pos = draw_base_pos(jax.random.fold_in(jax.random.fold_in(key_of[17], part), 71), part)
    centers = jnp.clip(jax.random.uniform(key_of[5], (3, CTRL), jnp.float32, 0.0, 1.0), 0.0, 1.0)
    amplitudes = normal_values(key_of[6], (3, CTRL), 0.05, 0.3, (), jnp.float32)
    edge_in = normal_values(key_of[7], (3 * LATENT, LATENT), (3 * LATENT) ** -0.5, 0.3125)
    edge_geo = normal_values(key_of[8], (4, LATENT), 4 ** -0.5, 3.0, (), jnp.float32)
    edge_out = normal_values(key_of[9], (LATENT, LATENT), LATENT ** -0.5, 0.5)
    edge_gain = jnp.clip(1.0 + 0.1 * jax.random.normal(key_of[10], (LATENT,), jnp.float32), 0.5, 1.5)
    node_in = normal_values(key_of[11], (2 * LATENT, LATENT), (2 * LATENT) ** -0.5, 0.375)
    node_out = normal_values(key_of[12], (LATENT, LATENT), LATENT ** -0.5, 0.5)
    node_gain = jnp.clip(1.0 + 0.1 * jax.random.normal(key_of[13], (LATENT,), jnp.float32), 0.5, 1.5)
    senders = draw_senders(jax.random.fold_in(jax.random.fold_in(key_of[17], part), 71), part)
    receivers = place_ends(jax.random.randint(own_keys[15], (EDGES,), 0, NV_DEV), jax.random.fold_in(own_keys[15], 1), 0, NV_DEV - 1).astype(jnp.int32)
    send_rows = place_ends(jax.random.randint(own_keys[16], (N_DOM, N_DOM, HALO), 0, NV_DEV), jax.random.fold_in(own_keys[16], 1), 0, NV_DEV - 1).astype(jnp.int32)
    return dict(node_latent=node_latent, edge_latent=edge_latent, node_cot=node_cot, edge_cot=edge_cot, base_pos=base_pos, centers=centers, amplitudes=amplitudes, edge_in=edge_in, edge_geo=edge_geo, edge_out=edge_out, edge_gain=edge_gain, node_in=node_in, node_out=node_out, node_gain=node_gain, senders=senders, receivers=receivers, send_rows=send_rows)


RBF_RATE = 78.125
exact_mode = lax.Precision.HIGHEST

def radial(points, centers):
    squared = jnp.zeros((points.shape[1], centers.shape[1]), jnp.float32)
    for component in range(3):
        offset_k = points[component][:, None] - centers[component][None, :]
        squared = squared + offset_k * offset_k
    return jnp.exp(-RBF_RATE * squared)

def layer_norm(values, gain):
    centred = values - lax.optimization_barrier(jnp.mean(values, axis=-1, keepdims=True))
    spread_inv = lax.rsqrt(lax.optimization_barrier(jnp.mean(centred * centred, axis=-1, keepdims=True)) + 1e-05)
    return centred * spread_inv * gain

def norm_back(values, gain, upstream):
    centred = values - lax.optimization_barrier(jnp.mean(values, axis=-1, keepdims=True))
    spread_inv = lax.rsqrt(lax.optimization_barrier(jnp.mean(centred * centred, axis=-1, keepdims=True)) + 1e-05)
    normed = centred * spread_inv
    scaled = upstream * gain
    return spread_inv * (scaled - lax.optimization_barrier(jnp.mean(scaled, axis=-1, keepdims=True)) - normed * lax.optimization_barrier(jnp.mean(scaled * normed, axis=-1, keepdims=True)))

def silu_slope(values):
    sigma = jax.nn.sigmoid(values)
    return sigma * (1.0 + values * (1.0 - sigma))

def reference(node_latent, edge_latent, node_cot, edge_cot, base_pos, centers, amplitudes, edge_in, edge_geo, edge_out, edge_gain, node_in, node_out, node_gain, senders, receivers, send_rows):
    width = node_latent.shape[1]
    edge_ids = jnp.arange(EDGES, dtype=jnp.int32)
    edge_home = (edge_ids // NE_DEV).astype(jnp.int32)
    recv_global = (edge_home * NV_DEV + receivers).astype(jnp.int32)
    is_local = senders < NV_DEV
    slot_index = jnp.maximum(senders - NV_DEV, 0).astype(jnp.int32)
    source_part = jnp.minimum(slot_index // HALO, N_DOM - 1).astype(jnp.int32)
    halo_row = send_rows[source_part, edge_home, slot_index % HALO]
    send_global = jnp.where(is_local, edge_home * NV_DEV + senders, source_part * NV_DEV + halo_row).astype(jnp.int32)
    base_blocks = jnp.transpose(base_pos.reshape(3, N_DOM, NV_DEV), (1, 0, 2))

    def place_block(block):
        return block + jnp.einsum('kc,nc->kn', amplitudes, radial(block, centers), precision=exact_mode)
    placed = jnp.transpose(lax.map(place_block, base_blocks), (1, 0, 2)).reshape(3, NODES)
    w_send = edge_in[:width]
    w_recv = edge_in[width:2 * width]
    w_edge = edge_in[2 * width:]
    w_node = node_in[:width]
    w_agg = node_in[width:]
    h_send = node_latent[send_global]
    h_recv = node_latent[recv_global]
    delta = placed[:, send_global] - placed[:, recv_global]
    length = jnp.sqrt(lax.optimization_barrier(jnp.sum(delta * delta, axis=0)) + 0.01)
    geometry = jnp.concatenate([delta, length[None, :]], axis=0)
    pre_act = jnp.dot(h_send, w_send, preferred_element_type=jnp.float32) + jnp.dot(h_recv, w_recv, preferred_element_type=jnp.float32) + jnp.dot(edge_latent, w_edge, preferred_element_type=jnp.float32) + jnp.einsum('ke,kl->el', geometry, edge_geo, precision=exact_mode)
    hidden = jax.nn.silu(pre_act).astype(jnp.bfloat16)
    edge_mid = jnp.dot(hidden, edge_out, preferred_element_type=jnp.float32)
    updated = (edge_latent.astype(jnp.float32) + layer_norm(edge_mid, edge_gain)).astype(jnp.bfloat16)
    aggregate = jax.ops.segment_sum(updated.astype(jnp.float32), recv_global, NODES).astype(jnp.bfloat16)
    node_pre = jnp.dot(node_latent, w_node, preferred_element_type=jnp.float32) + jnp.dot(aggregate, w_agg, preferred_element_type=jnp.float32)
    node_hidden = jax.nn.silu(node_pre).astype(jnp.bfloat16)
    node_mid = jnp.dot(node_hidden, node_out, preferred_element_type=jnp.float32)
    grad_mid = norm_back(node_mid, node_gain, node_cot.astype(jnp.float32)).astype(jnp.bfloat16)
    grad_pre = (jnp.dot(grad_mid, node_out.T, preferred_element_type=jnp.float32) * silu_slope(node_pre)).astype(jnp.bfloat16)
    grad_agg = jnp.dot(grad_pre, w_agg.T, preferred_element_type=jnp.float32).astype(jnp.bfloat16)
    grad_upd = edge_cot.astype(jnp.float32) + grad_agg[recv_global].astype(jnp.float32)
    grad_emid = norm_back(edge_mid, edge_gain, grad_upd).astype(jnp.bfloat16)
    grad_epre = jnp.dot(grad_emid, edge_out.T, preferred_element_type=jnp.float32) * silu_slope(pre_act)
    grad_eb = grad_epre.astype(jnp.bfloat16)
    grad_edges = grad_upd + jnp.dot(grad_eb, w_edge.T, preferred_element_type=jnp.float32)
    grad_snd = jnp.dot(grad_eb, w_send.T, preferred_element_type=jnp.float32).astype(jnp.bfloat16)
    grad_rcv = jnp.dot(grad_eb, w_recv.T, preferred_element_type=jnp.float32).astype(jnp.bfloat16)
    grad_geo = jnp.einsum('el,kl->ke', grad_epre, edge_geo, precision=exact_mode)
    grad_delta = grad_geo[:3] + grad_geo[3][None, :] * delta / length[None, :]
    grad_nodes = node_cot.astype(jnp.float32) + jnp.dot(grad_pre, w_node.T, preferred_element_type=jnp.float32) + jax.ops.segment_sum(grad_snd.astype(jnp.float32), send_global, NODES) + jax.ops.segment_sum(grad_rcv.astype(jnp.float32), recv_global, NODES)
    grad_pos = jax.ops.segment_sum(grad_delta.T, send_global, NODES).T - jax.ops.segment_sum(grad_delta.T, recv_global, NODES).T
    grad_blocks = jnp.transpose(grad_pos.reshape(3, N_DOM, NV_DEV), (1, 0, 2))

    def amp_block(pair):
        block, grads = pair
        return jnp.einsum('kn,nc->kc', grads, radial(block, centers), precision=exact_mode)
    grad_controls = lax.optimization_barrier(jnp.sum(lax.map(amp_block, (base_blocks, grad_blocks)), axis=0))
    return (grad_nodes, grad_edges, grad_controls)
```

```python
import functools

import jax
import jax.numpy as jnp
from jax import lax
from jax.experimental import pallas as pl
from jax.experimental.pallas import tpu as pltpu
from jax.sharding import PartitionSpec as P

REACH = 2
RBF_RATE = 78.125
SCALE = (RBF_RATE * 1.4426950408889634) ** 0.5
FAR = 4.0 * SCALE
OFFSETS = [step for step in range(-REACH, REACH + 1) if step != 0]
NEAR = len(OFFSETS)
F32 = jnp.float32
BF16 = jnp.bfloat16
LANES = 128
VMEM_FULL = pl.BlockSpec(memory_space=pltpu.VMEM)
ANY = pl.BlockSpec(memory_space=pl.ANY)


def dot(a, b):
    return jnp.dot(a, b, preferred_element_type=F32)


def dot_t(a, b):
    return lax.dot_general(a, b, (((1,), (1,)), ((), ())), preferred_element_type=F32)


def stack_rows(rows, height):
    at = lax.broadcasted_iota(jnp.int32, (height, rows[0].shape[1]), 0)
    out = jnp.zeros(at.shape, F32)
    for k, row in enumerate(rows):
        if row is not None:
            out = jnp.where(at == k, row, out)
    return out


def split(x):
    hi = x.astype(BF16)
    return hi, (x - hi.astype(F32)).astype(BF16)


def three(x):
    hi = x.astype(BF16).astype(F32)
    rest = x - hi
    mid = rest.astype(BF16).astype(F32)
    return hi, mid, rest - mid


def as_columns(row):
    wide = jnp.broadcast_to(row.astype(F32), (LANES, row.shape[1])).astype(BF16)
    return jnp.transpose(wide)


def lane_iota(shape):
    return lax.broadcasted_iota(jnp.int32, shape, 1).astype(F32).astype(BF16)


def tiles_match(key, count):
    one, zero = jnp.ones_like(key), jnp.zeros_like(key)
    return jnp.concatenate(
        [jnp.where(key == jnp.full_like(key, j), one, zero) for j in range(count)], axis=1
    )


def columns_match(row, width):
    within = as_columns(row % LANES)
    tile = as_columns(row // LANES)
    key = jnp.where(within == lane_iota(within.shape), tile, jnp.full_like(tile, -1.0))
    return tiles_match(key, width // LANES)


def rows_match(row, height):
    block = row.shape[1]
    group = row // 16
    at = lax.broadcasted_iota(jnp.int32, (16, block), 0)
    key = jnp.where(at == row - group * 16, group, -1).astype(F32).astype(BF16)
    one, zero = jnp.ones_like(key), jnp.zeros_like(key)
    return jnp.concatenate(
        [jnp.where(key == jnp.full_like(key, q), one, zero) for q in range(height // 16)], axis=0
    )


def lane_gather(table_ref, row, count):
    block = row.shape[1]
    lane = jnp.broadcast_to(row % LANES, (8, block))
    tile = jnp.broadcast_to(row // LANES, (8, block))
    pieces = []
    for j in range(block // LANES):
        here = slice(j * LANES, (j + 1) * LANES)
        out = jnp.zeros((8, LANES), F32)
        for c in range(count):
            source = table_ref[:, c * LANES : (c + 1) * LANES]
            taken = jnp.take_along_axis(source, lane[:, here], axis=1, mode="promise_in_bounds")
            out = jnp.where(tile[:, here] == c, taken, out)
        pieces.append(out)
    return jnp.concatenate(pieces, axis=1)


def compact_row(raw, nodes, slots):
    me = lax.axis_index("dom")
    slot = jnp.maximum(raw - nodes, 0)
    off = slot // slots - me
    near = jnp.clip(jnp.where(off < 0, off + REACH, off + REACH - 1), 0, NEAR - 1)
    return jnp.where(raw >= nodes, nodes + near * slots + slot % slots, raw)


def neighbours(parts):
    me = lax.axis_index("dom")
    out = []
    for off in OFFSETS:
        there = me + off
        inside = (there >= 0) & (there < parts)
        out.append((inside, lax.rem(there + parts, parts)))
    return out


def remote(src, dst, send_sem, recv_sem, partner):
    return pltpu.make_async_remote_copy(
        src_ref=src,
        dst_ref=dst,
        send_sem=send_sem,
        recv_sem=recv_sem,
        device_id={"dom": partner},
        device_id_type=pl.DeviceIdType.MESH,
    )


def start_kernel(
    parts,
    lat_ref,
    pos_ref,
    cen_ref,
    amp_ref,
    rows_ref,
    halo_ref,
    place_ref,
    phi_ref,
    out_s,
    pout_s,
    pin_s,
    base_s,
    cmat_s,
    phi_s,
    send_sem,
    recv_sem,
    psend_sem,
    precv_sem,
    phi_sem,
):
    nodes = lat_ref.shape[0]
    slots = rows_ref.shape[2]
    controls = cen_ref.shape[1]
    partners = neighbours(parts)
    barrier = pltpu.get_barrier_semaphore()
    for inside, partner in partners:

        @pl.when(inside)
        def _():
            pl.semaphore_signal(
                barrier, inc=1, device_id={"dom": partner}, device_id_type=pl.DeviceIdType.MESH
            )

    rows = [rows_ref[0, pl.ds(partner, 1), :] for _, partner in partners]
    base_s[...] = stack_rows([pos_ref[k : k + 1, :] for k in range(3)], 8)
    match = columns_match(jnp.concatenate(rows, axis=1), nodes)
    taken = dot(match, lat_ref[...]).astype(BF16)
    for k in range(NEAR):
        out_s[k] = taken[k * slots : (k + 1) * slots]
        pout_s[k] = lane_gather(base_s, rows[k], nodes // LANES)
    for k, (inside, _) in enumerate(partners):

        @pl.when(jnp.logical_not(inside))
        def _():
            halo_ref[k] = jnp.zeros_like(halo_ref[k])
            pin_s[k] = jnp.zeros_like(pin_s[k])

    def copies(k):
        there = NEAR - 1 - k
        partner = partners[k][1]
        return (
            remote(out_s.at[k], halo_ref.at[there], send_sem.at[k], recv_sem.at[there], partner),
            remote(pout_s.at[k], pin_s.at[there], psend_sem.at[k], precv_sem.at[there], partner),
        )

    pl.semaphore_wait(barrier, sum(inside.astype(jnp.int32) for inside, _ in partners))

    for k, (inside, _) in enumerate(partners):

        @pl.when(inside)
        def _():
            for copy in copies(k):
                copy.start()

    cen = [SCALE * (cen_ref[k : k + 1, :] - 0.5) for k in range(3)]
    crows = []
    for k in range(3):
        hi, mid, low = three(cen[k])
        crows += [hi, mid, hi, low, mid, hi]
    ones = jnp.ones_like(cen[0])
    crows += [ones, ones, ones]
    crows += list(three(-(cen[0] * cen[0] + cen[1] * cen[1] + cen[2] * cen[2])))
    cmat_s[...] = jnp.concatenate(
        [stack_rows(crows[j : j + 8], 8) for j in range(0, 24, 8)]
        + [jnp.zeros((LANES - 24, controls), F32)],
        axis=0,
    ).astype(BF16)
    amp = stack_rows([amp_ref[k : k + 1, :] for k in range(3)], 8)
    amp_hi = amp.astype(BF16).astype(F32)
    amp16 = jnp.concatenate([amp_hi, amp - amp_hi], axis=0).astype(BF16)

    def radial(base, first, size, index):
        moved = jnp.clip(SCALE * (base - 0.5), -FAR, FAR)
        parts_of = [three(moved[k : k + 1]) for k in range(3)]
        prows = []
        for hi, mid, low in parts_of:
            hi2, mid2, low2 = 2.0 * hi, 2.0 * mid, 2.0 * low
            prows += [hi2, hi2, mid2, hi2, mid2, low2]
        norm = moved[0:1] * moved[0:1] + moved[1:2] * moved[1:2] + moved[2:3] * moved[2:3]
        prows += list(three(-norm))
        one = jnp.ones_like(norm)
        prows += [one, one, one]
        wide = jnp.concatenate(
            [stack_rows(prows[j : j + 8], 8) for j in range(0, 24, 8)]
            + [jnp.zeros((LANES - 24, size), F32)],
            axis=0,
        )
        left = jnp.transpose(wide).astype(BF16)
        phi = jnp.exp2(dot(left, cmat_s[...])).astype(BF16)
        phi_s[pl.ds(first, size), :] = phi
        shift = dot_t(amp16, phi)
        place_ref[:, pl.ds(first, size)] = base + (shift[0:8] + shift[8:16])
        pltpu.make_async_copy(
            phi_s.at[pl.ds(first, size)], phi_ref.at[pl.ds(first, size)], phi_sem.at[index]
        ).start()

    size = 256
    own = nodes // size

    def own_step(i, carry):
        first = pl.multiple_of(i * size, size)
        radial(base_s[:, pl.ds(first, size)], first, size, i)
        return carry

    lax.fori_loop(0, own, own_step, 0)
    for k, (inside, _) in enumerate(partners):

        @pl.when(inside)
        def _():
            for copy in copies(NEAR - 1 - k):
                copy.wait_recv()

    pair = size // slots
    for j in range(NEAR // pair):
        halo = jnp.concatenate([pin_s[j * pair + i] for i in range(pair)], axis=1)
        radial(halo, nodes + j * size, size, own + j)
    for k, (inside, _) in enumerate(partners):

        @pl.when(inside)
        def _():
            for copy in copies(k):
                copy.wait_send()

    for i in range(own + NEAR // pair):
        here = pl.ds(i * size, size)
        pltpu.make_async_copy(phi_s.at[here], phi_ref.at[here], phi_sem.at[i]).wait()


def start(node_latent, base_pos, centers, amplitudes, send_rows, parts):
    nodes, width = node_latent.shape
    slots = send_rows.shape[2]
    controls = centers.shape[1]
    every = nodes + NEAR * slots
    return pl.pallas_call(
        functools.partial(start_kernel, parts),
        in_specs=[VMEM_FULL] * 5,
        out_specs=[VMEM_FULL, VMEM_FULL, ANY],
        out_shape=[
            jax.ShapeDtypeStruct((NEAR, slots, width), BF16),
            jax.ShapeDtypeStruct((8, every), F32),
            jax.ShapeDtypeStruct((every, controls), BF16),
        ],
        scratch_shapes=[
            pltpu.VMEM((NEAR, slots, width), BF16),
            pltpu.VMEM((NEAR, 8, slots), F32),
            pltpu.VMEM((NEAR, 8, slots), F32),
            pltpu.VMEM((8, nodes), F32),
            pltpu.VMEM((LANES, controls), BF16),
            pltpu.VMEM((every, controls), BF16),
            pltpu.SemaphoreType.DMA((NEAR,)),
            pltpu.SemaphoreType.DMA((NEAR,)),
            pltpu.SemaphoreType.DMA((NEAR,)),
            pltpu.SemaphoreType.DMA((NEAR,)),
            pltpu.SemaphoreType.DMA((every // 256,)),
        ],
        compiler_params=pltpu.CompilerParams(collective_id=0, has_side_effects=True),
        name="start",
    )(node_latent, base_pos, centers, amplitudes, send_rows)


def normed_of(values):
    centred = values - jnp.mean(values, axis=-1, keepdims=True)
    inv = lax.rsqrt(jnp.mean(centred * centred, axis=-1, keepdims=True) + 1e-05)
    return centred * inv, inv


def norm_back(values, gain, upstream):
    normed, inv = normed_of(values)
    scaled = upstream * gain
    return inv * (
        scaled
        - jnp.mean(scaled, axis=-1, keepdims=True)
        - normed * jnp.mean(scaled * normed, axis=-1, keepdims=True)
    )


def sigmoid(values):
    return 0.5 * jnp.tanh(0.5 * values) + 0.5


def paired(values, weights):
    half = values.shape[0] // 2
    out = dot(jnp.concatenate([values[:half], values[half:]], axis=1), weights)
    return jnp.concatenate([out[:, :LANES], out[:, LANES:]], axis=0)


def picked(pair, second):
    pair = pair.astype(BF16)
    return jnp.where(second, pair[:, LANES:], pair[:, :LANES])


def halves(values, second):
    zero = jnp.zeros_like(values)
    return jnp.concatenate([jnp.where(second, zero, values), jnp.where(second, values, zero)], axis=1)


def edges_kernel(
    sidx_ref,
    ridx_ref,
    lat_ref,
    halo_ref,
    place_ref,
    phi_ref,
    elat_ref,
    ecot_ref,
    ncot_ref,
    ein_ref,
    egeo_ref,
    eout_ref,
    egain_ref,
    nin_ref,
    nout_ref,
    ngain_ref,
    gedge_ref,
    ghid_ref,
    gnode_ref,
    ctrl_ref,
    phi_s,
    phi_sem,
    stab_s,
    rtab_s,
    gtab_s,
    win_s,
    wout_s,
    woutt_s,
    wback_s,
    slope_s,
    normed_s,
    rkey_s,
    rtile_s,
    stile_s,
    unit_s,
    agg_s,
    sgeo_s,
    rgeo_s,
):
    phase = pl.program_id(0)
    step = pl.program_id(1)
    last = pl.num_programs(1) - 1
    nodes, width = lat_ref.shape
    away = halo_ref.shape[0]
    every = nodes + away
    slots = away // NEAR
    block = elat_ref.shape[0]
    at = pl.ds(pl.multiple_of(step * block, block), block)
    shalf = every // 2
    rhalf = nodes // 2
    load_phi = pltpu.make_async_copy(phi_ref, phi_s, phi_sem)

    @pl.when((phase == 0) & (step == 0))
    def _():
        load_phi.start()
        agg_s[...] = jnp.zeros_like(agg_s)
        sgeo_s[...] = jnp.zeros_like(sgeo_s)
        rgeo_s[...] = jnp.zeros_like(rgeo_s)
        stab_s[:, :width] = lat_ref[:shalf]
        stab_s[: nodes - shalf, width:] = lat_ref[shalf:]
        stab_s[nodes - shalf :, width:] = halo_ref[...]
        rtab_s[:, :width] = lat_ref[:rhalf]
        rtab_s[:, width:] = lat_ref[rhalf:]
        geo = stack_rows([egeo_ref[k : k + 1, :] for k in range(4)], 8)
        hi = geo.astype(BF16).astype(F32)
        win_s[: 3 * width] = ein_ref[...]
        win_s[3 * width :] = jnp.concatenate(
            [hi + pltpu.roll(hi, 4, 0), geo - hi, jnp.zeros((LANES - 16, width), F32)], axis=0
        ).astype(BF16)
        w_out = eout_ref[...]
        zero = jnp.zeros_like(w_out)
        turned = jnp.transpose(w_out.astype(F32)).astype(BF16)
        wout_s[...] = jnp.concatenate(
            [jnp.concatenate([w_out, zero], axis=1), jnp.concatenate([zero, w_out], axis=1)], axis=0
        )
        woutt_s[...] = jnp.concatenate(
            [jnp.concatenate([turned, zero], axis=1), jnp.concatenate([zero, turned], axis=1)],
            axis=0,
        )
        w_edge = jnp.transpose(ein_ref[2 * width :].astype(F32)).astype(BF16)
        third = egeo_ref[3:4, :]
        spread = stack_rows(
            [egeo_ref[k : k + 1, :] for k in range(3)] + [None, third, third, third], 8
        )
        spread = jnp.transpose(jnp.concatenate([spread] * (LANES // 8), axis=0)).astype(BF16)
        wback_s[...] = jnp.concatenate(
            [
                jnp.concatenate([w_edge, spread], axis=1),
                jnp.concatenate([zero, spread], axis=1),
            ],
            axis=0,
        )

    @pl.when(phase == 0)
    def _():
        srow = compact_row(sidx_ref[0], nodes, slots)
        rrow = ridx_ref[0]
        delta = lane_gather(place_ref, srow, every // LANES) - lane_gather(
            place_ref, rrow, nodes // LANES
        )
        length = jnp.sqrt(jnp.sum(delta * delta, axis=0, keepdims=True) + 0.01)
        level = lax.broadcasted_iota(jnp.int32, delta.shape, 0)
        geo = jnp.where(level == 3, length, delta)
        hi = geo.astype(BF16).astype(F32)
        wide = jnp.concatenate(
            [hi + pltpu.roll(geo - hi, 4, 0), hi, jnp.zeros((LANES - 16, block), F32)], axis=0
        ).astype(BF16)
        geo_cols = jnp.transpose(wide)
        unit = jnp.where(level < 3, 1.0, pltpu.roll(delta * (1.0 / length), 4, 0)).astype(F32)
        unit_s[at, :] = jnp.transpose(
            jnp.concatenate([unit] * (LANES // 8), axis=0).astype(BF16)
        )

        lane = lane_iota((block, LANES))
        none = jnp.full_like(lane, -1.0)
        stile = as_columns(srow // LANES)
        second = stile >= jnp.full_like(stile, shalf // LANES)
        local = jnp.where(second, stile - jnp.full_like(stile, shalf // LANES), stile)
        skey = jnp.where(as_columns(srow % LANES) == lane, local, none)
        sent = picked(dot(tiles_match(skey, shalf // LANES), stab_s[...]), second)
        rtile = as_columns(rrow // LANES)
        upper = rtile >= jnp.full_like(rtile, rhalf // LANES)
        local = jnp.where(upper, rtile - jnp.full_like(rtile, rhalf // LANES), rtile)
        rkey = jnp.where(as_columns(rrow % LANES) == lane, local, none)
        got = picked(dot(tiles_match(rkey, rhalf // LANES), rtab_s[...]), upper)
        stile_s[at, :] = stile
        rtile_s[at, :] = rtile
        rkey_s[at, :] = rkey

        latent = elat_ref[...]
        pre = dot(jnp.concatenate([sent, got, latent, geo_cols], axis=1), win_s[...])
        sigma = sigmoid(pre)
        hidden = pre * sigma
        slope = sigma + hidden * (1.0 - sigma)
        normed, inv = normed_of(paired(hidden.astype(BF16), wout_s[...]))
        slope_s[at, :] = slope * inv
        normed_s[at, :] = normed
        updated = (latent.astype(F32) + normed * egain_ref[...]).astype(BF16)
        agg_s[...] += dot(rows_match(rrow % rhalf, rhalf), halves(updated, upper))

    @pl.when((phase == 0) & (step == last))
    def _():
        latent = lat_ref[...]
        w_node = nin_ref[:width, :]
        w_agg = nin_ref[width:, :]
        cot = ncot_ref[...].astype(F32)
        agg = jnp.concatenate([agg_s[:, :width], agg_s[:, width:]], axis=0).astype(BF16)
        node_pre = dot(jnp.concatenate([latent, agg], axis=1), nin_ref[...])
        sigma = sigmoid(node_pre)
        hidden = node_pre * sigma
        node_mid = dot(hidden.astype(BF16), nout_ref[...])
        grad_mid = norm_back(node_mid, ngain_ref[...], cot).astype(BF16)
        grad_pre = (
            dot_t(grad_mid, nout_ref[...]) * (sigma + hidden * (1.0 - sigma))
        ).astype(BF16)
        gagg = dot_t(grad_pre, w_agg).astype(BF16)
        gtab_s[...] = jnp.concatenate([gagg[:rhalf], gagg[rhalf:]], axis=1)
        gnode_ref[...] = cot + dot_t(grad_pre, w_node)

    @pl.when(phase == 1)
    def _():
        rtile = rtile_s[at, :]
        stile = stile_s[at, :]
        normed = normed_s[at, :]
        upper = rtile >= jnp.full_like(rtile, rhalf // LANES)
        spread = picked(dot(tiles_match(rkey_s[at, :], rhalf // LANES), gtab_s[...]), upper)
        grad_upd = ecot_ref[...].astype(F32) + spread.astype(F32)
        scaled = grad_upd * egain_ref[...]
        inner = (
            scaled
            - jnp.mean(scaled, axis=-1, keepdims=True)
            - normed * jnp.mean(scaled * normed, axis=-1, keepdims=True)
        )
        grad_pre = paired(inner.astype(BF16), woutt_s[...]) * slope_s[at, :]
        hi, lo = split(grad_pre)
        ghid_ref[...] = hi
        back = dot(jnp.concatenate([hi, lo], axis=1), wback_s[...])
        gedge_ref[...] = grad_upd + back[:, :width]
        moved = (back[:, width:] * unit_s[at, :].astype(F32)).astype(BF16)
        holder = (lax.broadcasted_iota(jnp.int32, (block, LANES), 1) // 8).astype(F32).astype(BF16)
        zero = jnp.zeros_like(moved)
        srow = compact_row(sidx_ref[0], nodes, slots)
        rrow = ridx_ref[0]
        sgeo_s[...] += dot(rows_match(srow % LANES, LANES), jnp.where(holder == stile, moved, zero))
        rgeo_s[...] += dot(rows_match(rrow % LANES, LANES), jnp.where(holder == rtile, moved, zero))

    @pl.when((phase == 1) & (step == last))
    def _():
        load_phi.wait()
        sgeo = jnp.transpose(sgeo_s[...])
        rgeo = jnp.transpose(rgeo_s[...])
        tiles = []
        for t in range(every // LANES):
            tile = sgeo[8 * t : 8 * t + 8]
            if t < nodes // LANES:
                tile = tile - rgeo[8 * t : 8 * t + 8]
            tiles.append(tile + pltpu.roll(tile, 4, 0))
        gpos = jnp.concatenate(tiles, axis=1)
        gpos = jnp.where(lax.broadcasted_iota(jnp.int32, gpos.shape, 0) < 3, gpos, 0.0)
        hi = gpos.astype(BF16).astype(F32)
        both = jnp.concatenate([hi, gpos - hi], axis=0).astype(BF16)
        amp = dot(both, phi_s[...])
        amp = amp[0:8] + amp[8:16]
        for j in range(ctrl_ref.shape[0]):
            ctrl_ref[j] = amp[0:4, j * LANES : (j + 1) * LANES]


def edges(senders, receivers, lat, halo, place, phi, edge_latent, edge_cot, node_cot, weights):
    count, width = edge_latent.shape
    block = 1024 if count % 1024 == 0 else 512
    turns = count // block
    nodes = lat.shape[0]
    away = halo.shape[0]
    every = nodes + away
    controls = phi.shape[1]
    full = lambda shape: pl.BlockSpec(shape, lambda p, i: (0,) * len(shape))
    index_spec = pl.BlockSpec((1, 1, block), lambda p, i: (i, 0, 0))
    second = pl.BlockSpec((block, width), lambda p, i: (i * p, 0))
    chunks = (controls // LANES, 4, LANES)
    return pl.pallas_call(
        edges_kernel,
        grid=(2, turns),
        in_specs=[
            index_spec,
            index_spec,
            full(lat.shape),
            full(halo.shape),
            full(place.shape),
            ANY,
            pl.BlockSpec((block, width), lambda p, i: (i * (1 - p), 0)),
            second,
            full(node_cot.shape),
        ]
        + [full(w.shape) for w in weights],
        out_specs=[second, second, full((nodes, width)), full(chunks)],
        out_shape=[
            jax.ShapeDtypeStruct((count, width), F32),
            jax.ShapeDtypeStruct((count, width), BF16),
            jax.ShapeDtypeStruct((nodes, width), F32),
            jax.ShapeDtypeStruct(chunks, F32),
        ],
        scratch_shapes=[
            pltpu.VMEM((every, controls), BF16),
            pltpu.SemaphoreType.DMA,
            pltpu.VMEM((every // 2, 2 * width), BF16),
            pltpu.VMEM((nodes // 2, 2 * width), BF16),
            pltpu.VMEM((nodes // 2, 2 * width), BF16),
            pltpu.VMEM((3 * width + LANES, width), BF16),
            pltpu.VMEM((2 * width, 2 * width), BF16),
            pltpu.VMEM((2 * width, 2 * width), BF16),
            pltpu.VMEM((2 * width, width + LANES), BF16),
            pltpu.VMEM((count, width), F32),
            pltpu.VMEM((count, width), F32),
            pltpu.VMEM((count, LANES), BF16),
            pltpu.VMEM((count, LANES), BF16),
            pltpu.VMEM((count, LANES), BF16),
            pltpu.VMEM((count, LANES), BF16),
            pltpu.VMEM((nodes // 2, 2 * width), F32),
            pltpu.VMEM((LANES, LANES), F32),
            pltpu.VMEM((LANES, LANES), F32),
        ],
        compiler_params=pltpu.CompilerParams(
            dimension_semantics=("arbitrary", "arbitrary")
        ),
        name="edges",
    )(
        senders.reshape(turns, 1, block),
        receivers.reshape(turns, 1, block),
        lat,
        halo,
        place,
        phi,
        edge_latent,
        edge_cot,
        node_cot,
        *weights,
    )


def tail_kernel(
    parts,
    sidx_ref,
    ridx_ref,
    ghid_ref,
    gnode_ref,
    ctrl_ref,
    rows_ref,
    ein_ref,
    out_ref,
    amp_ref,
    sum_s,
    rsum_s,
    back_s,
    got_s,
    part_s,
    mine_s,
    all_s,
    back_send,
    back_recv,
    part_send,
    part_recv,
    all_send,
    all_recv,
):
    me = lax.axis_index("dom")
    turns, _, block = sidx_ref.shape
    nodes, width = gnode_ref.shape
    slots = rows_ref.shape[2]
    every = nodes + NEAR * slots
    shalf = every // 2
    rhalf = nodes // 2
    chunks = ctrl_ref.shape[0]
    reducers = max(r for r in range(1, parts + 1) if chunks % r == 0)
    per = chunks // reducers
    partners = neighbours(parts)
    others = [lax.rem(me + i, parts) for i in range(1, parts)]
    sources = [lax.rem(me + parts - i, parts) for i in range(1, parts)]
    barrier = pltpu.get_barrier_semaphore()
    for other in others:
        pl.semaphore_signal(
            barrier, inc=1, device_id={"dom": other}, device_id_type=pl.DeviceIdType.MESH
        )
    sum_s[...] = jnp.zeros_like(sum_s)
    rsum_s[...] = jnp.zeros_like(rsum_s)
    for k, (inside, _) in enumerate(partners):

        @pl.when(jnp.logical_not(inside))
        def _():
            got_s[k] = jnp.zeros_like(got_s[k])

    pl.semaphore_wait(barrier, parts - 1)

    def part_copy(i):
        other = others[i]
        return remote(
            ctrl_ref.at[pl.ds(jnp.minimum(other, reducers - 1) * per, per)],
            part_s.at[i],
            part_send.at[i],
            part_recv.at[i],
            other,
        )

    def all_copy(i):
        return remote(
            mine_s,
            all_s.at[pl.ds(jnp.minimum(me, reducers - 1) * per, per)],
            all_send.at[i],
            all_recv.at[i],
            others[i],
        )

    def when_reducer(device, run):
        if reducers == parts:
            run()
        else:
            pl.when(device < reducers)(run)

    for i in range(parts - 1):
        when_reducer(others[i], lambda: part_copy(i).start())

    def sender_step(t, carry):
        srow = compact_row(sidx_ref[t], nodes, slots)
        stile = as_columns(srow // LANES)
        second = stile >= jnp.full_like(stile, shalf // LANES)
        values = ghid_ref[pl.ds(pl.multiple_of(t * block, block), block), :]
        sum_s[...] += dot(rows_match(srow % shalf, shalf), halves(values, second))
        return carry

    lax.fori_loop(0, turns, sender_step, 0)
    w_send = ein_ref[:width]
    w_recv = ein_ref[width : 2 * width]

    def projected(values, weight):
        hi, lo = split(values)
        return dot_t(hi, weight) + dot_t(lo, weight)

    back = projected(sum_s[shalf - NEAR * slots :, width:], w_send).astype(BF16)
    for k in range(NEAR):
        back_s[k] = back[k * slots : (k + 1) * slots]

    def back_copy(k):
        there = NEAR - 1 - k
        return remote(
            back_s.at[k], got_s.at[there], back_send.at[k], back_recv.at[there], partners[k][1]
        )

    def reduce_mine():
        total = ctrl_ref[pl.ds(jnp.minimum(me, reducers - 1) * per, per)]
        for i in range(parts - 1):
            part_copy(i).wait_recv()
        for i in range(parts - 1):
            total = total + part_s[i]
        mine_s[...] = total
        all_s[pl.ds(jnp.minimum(me, reducers - 1) * per, per)] = total

    when_reducer(me, reduce_mine)
    for k, (inside, _) in enumerate(partners):

        @pl.when(inside)
        def _():
            back_copy(k).start()

    def send_all():
        for i in range(parts - 1):
            all_copy(i).start()

    when_reducer(me, send_all)

    def receiver_step(t, carry):
        rrow = ridx_ref[t]
        rtile = as_columns(rrow // LANES)
        upper = rtile >= jnp.full_like(rtile, rhalf // LANES)
        values = ghid_ref[pl.ds(pl.multiple_of(t * block, block), block), :]
        rsum_s[...] += dot(rows_match(rrow % rhalf, rhalf), halves(values, upper))
        return carry

    lax.fori_loop(0, turns, receiver_step, 0)
    sent = jnp.concatenate([sum_s[:, :width], sum_s[: nodes - shalf, width:]], axis=0)
    received = jnp.concatenate([rsum_s[:, :width], rsum_s[:, width:]], axis=0)
    total = gnode_ref[...] + projected(sent, w_send) + projected(received, w_recv)
    for k, (inside, _) in enumerate(partners):

        @pl.when(inside)
        def _():
            back_copy(NEAR - 1 - k).wait_recv()

    rows = jnp.concatenate([rows_ref[0, pl.ds(partner, 1), :] for _, partner in partners], axis=1)
    got = jnp.concatenate([got_s[k] for k in range(NEAR)], axis=0)
    out_ref[...] = total + dot(rows_match(rows, nodes), got)
    for k, (inside, _) in enumerate(partners):

        @pl.when(inside)
        def _():
            back_copy(k).wait_send()

    for i in range(parts - 1):
        when_reducer(others[i], lambda: part_copy(i).wait_send())
    when_reducer(me, lambda: [all_copy(i).wait_send() for i in range(parts - 1)] and None)
    for i in range(parts - 1):
        source = sources[i]

        def arrived():
            remote(
                mine_s,
                all_s.at[pl.ds(jnp.minimum(source, reducers - 1) * per, per)],
                all_send.at[i],
                all_recv.at[i],
                others[i],
            ).wait_recv()

        when_reducer(source, arrived)
    for j in range(chunks):
        amp_ref[:, j * LANES : (j + 1) * LANES] = all_s[j][0:3]


def tail(senders, receivers, ghid, gnode, ctrl, send_rows, edge_in, parts):
    count, width = ghid.shape
    block = 1024 if count % 1024 == 0 else 512
    turns = count // block
    nodes = gnode.shape[0]
    slots = send_rows.shape[2]
    every = nodes + NEAR * slots
    chunks = ctrl.shape[0]
    reducers = max(r for r in range(1, parts + 1) if chunks % r == 0)
    per = (chunks // reducers,) + ctrl.shape[1:]
    sems = pltpu.SemaphoreType.DMA((parts - 1,))
    return pl.pallas_call(
        functools.partial(tail_kernel, parts),
        in_specs=[VMEM_FULL] * 7,
        out_specs=[VMEM_FULL, VMEM_FULL],
        out_shape=[
            jax.ShapeDtypeStruct(gnode.shape, F32),
            jax.ShapeDtypeStruct((3, chunks * LANES), F32),
        ],
        scratch_shapes=[
            pltpu.VMEM((every // 2, 2 * width), F32),
            pltpu.VMEM((nodes // 2, 2 * width), F32),
            pltpu.VMEM((NEAR, slots, width), BF16),
            pltpu.VMEM((NEAR, slots, width), BF16),
            pltpu.VMEM((parts - 1,) + per, F32),
            pltpu.VMEM(per, F32),
            pltpu.VMEM(ctrl.shape, F32),
            pltpu.SemaphoreType.DMA((NEAR,)),
            pltpu.SemaphoreType.DMA((NEAR,)),
            sems,
            sems,
            sems,
            sems,
        ],
        compiler_params=pltpu.CompilerParams(collective_id=1, has_side_effects=True),
        name="tail",
    )(
        senders.reshape(turns, 1, block),
        receivers.reshape(turns, 1, block),
        ghid,
        gnode,
        ctrl,
        send_rows,
        edge_in,
    )


def shards(
    node_latent,
    edge_latent,
    node_cot,
    edge_cot,
    base_pos,
    centers,
    amplitudes,
    edge_in,
    edge_geo,
    edge_out,
    edge_gain,
    node_in,
    node_out,
    node_gain,
    senders,
    receivers,
    send_rows,
):
    parts = lax.axis_size("dom")
    width = node_latent.shape[1]
    halo, place, phi = start(node_latent, base_pos, centers, amplitudes, send_rows, parts)
    weights = (
        edge_in,
        edge_geo,
        edge_out,
        edge_gain[None, :],
        node_in,
        node_out,
        node_gain[None, :],
    )
    grad_edges, ghid, gnode, ctrl = edges(
        senders,
        receivers,
        node_latent,
        halo.reshape(-1, width),
        place,
        phi,
        edge_latent,
        edge_cot,
        node_cot,
        weights,
    )
    grad_nodes, grad_controls = tail(
        senders, receivers, ghid, gnode, ctrl, send_rows, edge_in, parts
    )
    return (grad_nodes, grad_edges, grad_controls)


def solution(mesh):
    split_rows = P(("groups", "dom"), None)
    in_specs = (
        split_rows,
        split_rows,
        split_rows,
        split_rows,
        P(None, ("groups", "dom")),
        P(),
        P(),
        P(),
        P(),
        P(),
        P(),
        P(),
        P(),
        P(),
        P(("groups", "dom")),
        P(("groups", "dom")),
        P(("groups", "dom"), None, None),
    )
    out_specs = (split_rows, split_rows, P("groups", None))
    return jax.shard_map(shards, mesh=mesh, in_specs=in_specs, out_specs=out_specs, check_vma=False)
```

```python
import functools

import jax
import jax.numpy as jnp
from jax import lax
from jax.experimental import pallas as pl
from jax.experimental.pallas import tpu as pltpu
from jax.sharding import PartitionSpec as P

REACH = 2
RBF_RATE = 78.125
SCALE = (RBF_RATE * 1.4426950408889634) ** 0.5
FAR = 4.0 * SCALE
OFFSETS = [step for step in range(-REACH, REACH + 1) if step != 0]
NEAR = len(OFFSETS)
F32 = jnp.float32
BF16 = jnp.bfloat16
LANES = 128
VMEM_FULL = pl.BlockSpec(memory_space=pltpu.VMEM)
ANY = pl.BlockSpec(memory_space=pl.ANY)


def dot(a, b):
    return jnp.dot(a, b, preferred_element_type=F32)


def dot_t(a, b):
    return lax.dot_general(a, b, (((1,), (1,)), ((), ())), preferred_element_type=F32)


def stack_rows(rows, height):
    at = lax.broadcasted_iota(jnp.int32, (height, rows[0].shape[1]), 0)
    out = jnp.zeros(at.shape, F32)
    for k, row in enumerate(rows):
        if row is not None:
            out = jnp.where(at == k, row, out)
    return out


def split(x):
    hi = x.astype(BF16)
    return hi, (x - hi.astype(F32)).astype(BF16)


def three(x):
    hi = x.astype(BF16).astype(F32)
    rest = x - hi
    mid = rest.astype(BF16).astype(F32)
    return hi, mid, rest - mid


def as_columns(row):
    wide = jnp.broadcast_to(row.astype(F32), (LANES, row.shape[1])).astype(BF16)
    return jnp.transpose(wide)


def lane_iota(shape):
    return lax.broadcasted_iota(jnp.int32, shape, 1).astype(F32).astype(BF16)


def tiles_match(key, count):
    one, zero = jnp.ones_like(key), jnp.zeros_like(key)
    return jnp.concatenate(
        [jnp.where(key == jnp.full_like(key, j), one, zero) for j in range(count)], axis=1
    )


def columns_match(row, width):
    within = as_columns(row % LANES)
    tile = as_columns(row // LANES)
    key = jnp.where(within == lane_iota(within.shape), tile, jnp.full_like(tile, -1.0))
    return tiles_match(key, width // LANES)


def rows_match(row, height):
    block = row.shape[1]
    group = row // 16
    at = lax.broadcasted_iota(jnp.int32, (16, block), 0)
    key = jnp.where(at == row - group * 16, group, -1).astype(F32).astype(BF16)
    one, zero = jnp.ones_like(key), jnp.zeros_like(key)
    return jnp.concatenate(
        [jnp.where(key == jnp.full_like(key, q), one, zero) for q in range(height // 16)], axis=0
    )


def lane_gather(table_ref, row, count):
    block = row.shape[1]
    lane = jnp.broadcast_to(row % LANES, (8, block))
    tile = jnp.broadcast_to(row // LANES, (8, block))
    pieces = []
    for j in range(block // LANES):
        here = slice(j * LANES, (j + 1) * LANES)
        out = jnp.zeros((8, LANES), F32)
        for c in range(count):
            source = table_ref[:, c * LANES : (c + 1) * LANES]
            taken = jnp.take_along_axis(source, lane[:, here], axis=1, mode="promise_in_bounds")
            out = jnp.where(tile[:, here] == c, taken, out)
        pieces.append(out)
    return jnp.concatenate(pieces, axis=1)


def compact_row(raw, nodes, slots):
    me = lax.axis_index("dom")
    slot = jnp.maximum(raw - nodes, 0)
    off = slot // slots - me
    near = jnp.clip(jnp.where(off < 0, off + REACH, off + REACH - 1), 0, NEAR - 1)
    return jnp.where(raw >= nodes, nodes + near * slots + slot % slots, raw)


def neighbours(parts):
    me = lax.axis_index("dom")
    out = []
    for off in OFFSETS:
        there = me + off
        inside = (there >= 0) & (there < parts)
        out.append((inside, lax.rem(there + parts, parts)))
    return out


def remote(src, dst, send_sem, recv_sem, partner):
    return pltpu.make_async_remote_copy(
        src_ref=src,
        dst_ref=dst,
        send_sem=send_sem,
        recv_sem=recv_sem,
        device_id={"dom": partner},
        device_id_type=pl.DeviceIdType.MESH,
    )


def copy_all(pairs, sems):
    copies = [
        pltpu.make_async_copy(source, target, sems.at[i]) for i, (source, target) in enumerate(pairs)
    ]
    for copy in copies:
        copy.start()
    return copies


def normed_of(values):
    centred = values - jnp.mean(values, axis=-1, keepdims=True)
    inv = lax.rsqrt(jnp.mean(centred * centred, axis=-1, keepdims=True) + 1e-05)
    return centred * inv, inv


def norm_back(values, gain, upstream):
    normed, inv = normed_of(values)
    scaled = upstream * gain
    return inv * (
        scaled
        - jnp.mean(scaled, axis=-1, keepdims=True)
        - normed * jnp.mean(scaled * normed, axis=-1, keepdims=True)
    )


def sigmoid(values):
    return 0.5 * jnp.tanh(0.5 * values) + 0.5


def paired(values, weights):
    half = values.shape[0] // 2
    out = dot(jnp.concatenate([values[:half], values[half:]], axis=1), weights)
    return jnp.concatenate([out[:, :LANES], out[:, LANES:]], axis=0)


def picked(pair, second):
    pair = pair.astype(BF16)
    return jnp.where(second, pair[:, LANES:], pair[:, :LANES])


def halves(values, second):
    zero = jnp.zeros_like(values)
    return jnp.concatenate([jnp.where(second, zero, values), jnp.where(second, values, zero)], axis=1)


def layer_kernel(parts, *refs):
    (
        lat_hbm,
        pos_hbm,
        cen_hbm,
        amp_hbm,
        rows_hbm,
        sidx_hbm,
        ridx_hbm,
        ein_hbm,
        egeo_hbm,
        eout_hbm,
        egain_hbm,
        nin_hbm,
        nout_hbm,
        ngain_hbm,
        elat_hbm,
        ecot_hbm,
        ncot_hbm,
        gedge_s,
        out_ref,
        amp_out,
        lat_ref,
        pos_ref,
        cen_ref,
        amp_ref,
        rows_ref,
        sidx_ref,
        ridx_ref,
        ein_ref,
        egeo_ref,
        eout_ref,
        egain_ref,
        nin_ref,
        nout_ref,
        ngain_ref,
        load_sem,
        halo_ref,
        place_ref,
        out_s,
        pout_s,
        pin_s,
        base_s,
        cmat_s,
        phi_s,
        send_sem,
        recv_sem,
        psend_sem,
        precv_sem,
        elat_s,
        ecot_s,
        ncot_s,
        ghid_s,
        gnode_s,
        elat_sem,
        ecot_sem,
        ncot_sem,
        stab_s,
        rtab_s,
        gtab_s,
        win_s,
        wout_s,
        woutt_s,
        wgeo_s,
        wedge_s,
        peer_s,
        wnode_s,
        slope_s,
        normed_s,
        rkey_s,
        rtile_s,
        stile_s,
        unit_s,
        agg_s,
        sgeo_s,
        rgeo_s,
        ctrl_ref,
        sum_s,
        rsum_s,
        back_s,
        got_s,
        part_s,
        mine_s,
        all_s,
        back_send,
        back_recv,
        part_send,
        part_recv,
        all_send,
        all_recv,
    ) = refs
    nodes = lat_ref.shape[0]
    slots = rows_ref.shape[2]
    controls = cen_ref.shape[1]
    partners = neighbours(parts)
    me = lax.axis_index("dom")
    others = [lax.rem(me + i, parts) for i in range(1, parts)]
    sources = [lax.rem(me + parts - i, parts) for i in range(1, parts)]
    barrier = pltpu.get_barrier_semaphore()
    for other in others:
        pl.semaphore_signal(
            barrier, inc=1, device_id={"dom": other}, device_id_type=pl.DeviceIdType.MESH
        )
    loads = copy_all(
        [
            (rows_hbm, rows_ref),
            (lat_hbm, lat_ref),
            (pos_hbm, pos_ref),
            (cen_hbm, cen_ref),
            (amp_hbm, amp_ref),
            (sidx_hbm, sidx_ref),
            (ridx_hbm, ridx_ref),
            (ein_hbm, ein_ref),
            (egeo_hbm, egeo_ref),
            (eout_hbm, eout_ref),
            (egain_hbm, egain_ref),
            (nin_hbm, nin_ref),
            (nout_hbm, nout_ref),
            (ngain_hbm, ngain_ref),
        ],
        load_sem,
    )
    width = lat_ref.shape[1]
    away = NEAR * slots
    every = nodes + away
    turns, _, block = sidx_ref.shape
    shalf = every // 2
    rhalf = nodes // 2

    def rows_of(t):
        return pl.ds(pl.multiple_of(t * block, block), block)

    def elat_copy(t):
        return pltpu.make_async_copy(elat_hbm.at[rows_of(t)], elat_s.at[rows_of(t)], elat_sem.at[t])

    def ecot_copy(t):
        return pltpu.make_async_copy(ecot_hbm.at[rows_of(t)], ecot_s.at[rows_of(t)], ecot_sem.at[t])

    for t in range(turns):
        elat_copy(t).start()
    load_ncot = pltpu.make_async_copy(ncot_hbm, ncot_s, ncot_sem)
    load_ncot.start()
    for t in range(turns):
        ecot_copy(t).start()
    for load in loads[:5]:
        load.wait()
    rows = [rows_ref[0, pl.ds(partner, 1), :] for _, partner in partners]
    base_s[...] = stack_rows([pos_ref[k : k + 1, :] for k in range(3)], 8)
    match = columns_match(jnp.concatenate(rows, axis=1), nodes)
    taken = dot(match, lat_ref[...]).astype(BF16)
    for k in range(NEAR):
        out_s[k] = taken[k * slots : (k + 1) * slots]
        pout_s[k] = lane_gather(base_s, rows[k], nodes // LANES)
    for k, (inside, _) in enumerate(partners):

        @pl.when(jnp.logical_not(inside))
        def _():
            halo_ref[k] = jnp.zeros_like(halo_ref[k])
            pin_s[k] = jnp.zeros_like(pin_s[k])

    def copies(k):
        there = NEAR - 1 - k
        partner = partners[k][1]
        return (
            remote(out_s.at[k], halo_ref.at[there], send_sem.at[k], recv_sem.at[there], partner),
            remote(pout_s.at[k], pin_s.at[there], psend_sem.at[k], precv_sem.at[there], partner),
        )

    cen = [SCALE * (cen_ref[k : k + 1, :] - 0.5) for k in range(3)]
    crows = []
    for k in range(3):
        hi, mid, low = three(cen[k])
        crows += [hi, mid, hi, low, mid, hi]
    ones = jnp.ones_like(cen[0])
    crows += [ones, ones, ones]
    crows += list(three(-(cen[0] * cen[0] + cen[1] * cen[1] + cen[2] * cen[2])))
    cmat_s[...] = jnp.concatenate(
        [stack_rows(crows[j : j + 8], 8) for j in range(0, 24, 8)]
        + [jnp.zeros((LANES - 24, controls), F32)],
        axis=0,
    ).astype(BF16)
    amp = stack_rows([amp_ref[k : k + 1, :] for k in range(3)], 8)
    amp_hi = amp.astype(BF16).astype(F32)
    amp16 = jnp.concatenate([amp_hi, amp - amp_hi], axis=0).astype(BF16)

    def radial(base, first, size, index=0):
        moved = jnp.clip(SCALE * (base - 0.5), -FAR, FAR)
        parts_of = [three(moved[k : k + 1]) for k in range(3)]
        prows = []
        for hi, mid, low in parts_of:
            hi2, mid2, low2 = 2.0 * hi, 2.0 * mid, 2.0 * low
            prows += [hi2, hi2, mid2, hi2, mid2, low2]
        norm = moved[0:1] * moved[0:1] + moved[1:2] * moved[1:2] + moved[2:3] * moved[2:3]
        prows += list(three(-norm))
        one = jnp.ones_like(norm)
        prows += [one, one, one]
        wide = jnp.concatenate(
            [stack_rows(prows[j : j + 8], 8) for j in range(0, 24, 8)]
            + [jnp.zeros((LANES - 24, size), F32)],
            axis=0,
        )
        left = jnp.transpose(wide).astype(BF16)
        phi = jnp.exp2(dot(left, cmat_s[...])).astype(BF16)
        phi_s[pl.ds(first, size), :] = phi
        shift = dot_t(amp16, phi)
        place_ref[:, pl.ds(first, size)] = base + (shift[0:8] + shift[8:16])

    size = 256
    own = nodes // size

    def own_step(i, carry):
        first = pl.multiple_of(i * size, size)
        radial(base_s[:, pl.ds(first, size)], first, size, i)
        return carry

    lax.fori_loop(0, own, own_step, 0)
    pl.semaphore_wait(barrier, parts - 1)

    for k, (inside, _) in enumerate(partners):

        @pl.when(inside)
        def _():
            for copy in copies(k):
                copy.start()

    for load in loads[5:]:
        load.wait()
    agg_s[...] = jnp.zeros_like(agg_s)
    sgeo_s[...] = jnp.zeros_like(sgeo_s)
    rgeo_s[...] = jnp.zeros_like(rgeo_s)
    stab_s[:, :width] = lat_ref[:shalf]
    stab_s[: nodes - shalf, width:] = lat_ref[shalf:]
    rtab_s[:, :width] = lat_ref[:rhalf]
    rtab_s[:, width:] = lat_ref[rhalf:]
    geo = stack_rows([egeo_ref[k : k + 1, :] for k in range(4)], 8)
    hi = geo.astype(BF16).astype(F32)
    win_s[: 3 * width] = ein_ref[...]
    win_s[3 * width :] = jnp.concatenate(
        [hi + pltpu.roll(hi, 4, 0), geo - hi, jnp.zeros((LANES - 16, width), F32)], axis=0
    ).astype(BF16)
    w_out = eout_ref[...]
    zero = jnp.zeros_like(w_out)
    turned = jnp.transpose(w_out.astype(F32)).astype(BF16)
    wout_s[...] = jnp.concatenate(
        [jnp.concatenate([w_out, zero], axis=1), jnp.concatenate([zero, w_out], axis=1)], axis=0
    )
    woutt_s[...] = jnp.concatenate(
        [jnp.concatenate([turned, zero], axis=1), jnp.concatenate([zero, turned], axis=1)],
        axis=0,
    )
    w_edge = jnp.transpose(ein_ref[2 * width :].astype(F32)).astype(BF16)
    third = egeo_ref[3:4, :]
    spread = stack_rows(
        [egeo_ref[k : k + 1, :] for k in range(3)] + [None, third, third, third], 8
    )
    spread = jnp.transpose(jnp.concatenate([spread] * (LANES // 8), axis=0)).astype(BF16)
    w_send = jnp.transpose(ein_ref[:width].astype(F32)).astype(BF16)
    w_recv = jnp.transpose(ein_ref[width : 2 * width].astype(F32)).astype(BF16)
    wnode_s[...] = jnp.concatenate([w_send, w_send, w_recv, w_recv], axis=0)
    wgeo_s[...] = jnp.concatenate(
        [jnp.concatenate([spread, zero], axis=1), jnp.concatenate([zero, spread], axis=1)], axis=0
    )
    wedge_s[...] = jnp.concatenate(
        [jnp.concatenate([w_edge, zero], axis=1), jnp.concatenate([zero, w_edge], axis=1)], axis=0
    )

    def upper_of(tile):
        return tile >= jnp.full_like(tile, rhalf // LANES)

    def receive(t, carry):
        at = rows_of(t)
        rrow = ridx_ref[t]
        rtile = as_columns(rrow // LANES)
        upper = upper_of(rtile)
        local = jnp.where(upper, rtile - jnp.full_like(rtile, rhalf // LANES), rtile)
        none = jnp.full_like(rtile, -1.0)
        rkey = jnp.where(as_columns(rrow % LANES) == lane_iota(rtile.shape), local, none)
        peer_s[at, :] = picked(dot(tiles_match(rkey, rhalf // LANES), rtab_s[...]), upper)
        rtile_s[at, :] = rtile
        rkey_s[at, :] = rkey
        return carry

    lax.fori_loop(0, turns, receive, 0)
    for k, (inside, _) in enumerate(partners):

        @pl.when(inside)
        def _():
            for copy in copies(NEAR - 1 - k):
                copy.wait_recv()

    pair = size // slots
    for j in range(NEAR // pair):
        halo = jnp.concatenate([pin_s[j * pair + i] for i in range(pair)], axis=1)
        radial(halo, nodes + j * size, size, own + j)
    for k in range(NEAR):
        stab_s[nodes - shalf + k * slots : nodes - shalf + (k + 1) * slots, width:] = halo_ref[k]

    sub = 256
    subs = block // sub

    def forward(t, carry):
        srow = compact_row(sidx_ref[t], nodes, slots)
        rrow = ridx_ref[t]
        elat_copy(t).wait()
        delta = lane_gather(place_ref, srow, every // LANES) - lane_gather(
            place_ref, rrow, nodes // LANES
        )
        length = jnp.sqrt(jnp.sum(delta * delta, axis=0, keepdims=True) + 0.01)
        level = lax.broadcasted_iota(jnp.int32, delta.shape, 0)
        geo = jnp.where(level == 3, length, delta)
        hi = geo.astype(BF16).astype(F32)
        wide = jnp.concatenate(
            [hi + pltpu.roll(geo - hi, 4, 0), hi, jnp.zeros((LANES - 16, block), F32)], axis=0
        ).astype(BF16)
        unit = jnp.where(level < 3, 1.0, pltpu.roll(delta * (1.0 / length), 4, 0)).astype(F32)
        unit = jnp.concatenate([unit] * (LANES // 8), axis=0).astype(BF16)
        lane = lane_iota((sub, LANES))
        none = jnp.full_like(lane, -1.0)

        def place_of(c):
            return pl.ds(pl.multiple_of(t * block + c * sub, sub), sub)

        def gathered(c):
            here = slice(c * sub, (c + 1) * sub)
            at = place_of(c)
            stile = as_columns(srow[:, here] // LANES)
            shift = jnp.full_like(stile, shalf // LANES)
            second = stile >= shift
            local = jnp.where(second, stile - shift, stile)
            skey = jnp.where(as_columns(srow[:, here] % LANES) == lane, local, none)
            sent = picked(dot(tiles_match(skey, shalf // LANES), stab_s[...]), second)
            stile_s[at, :] = stile
            unit_s[at, :] = jnp.transpose(unit[:, here])
            return jnp.concatenate(
                [sent, peer_s[at, :], elat_s[at, :], jnp.transpose(wide[:, here])], axis=1
            )

        def middle(c, joined):
            at = place_of(c)
            pre = dot(joined, win_s[...])
            sigma = sigmoid(pre)
            hidden = pre * sigma
            slope = sigma + hidden * (1.0 - sigma)
            normed, inv = normed_of(paired(hidden.astype(BF16), wout_s[...]))
            slope_s[at, :] = slope * inv
            normed_s[at, :] = normed
            latent = joined[:, 2 * width : 3 * width]
            updated = (latent.astype(F32) + normed * egain_ref[...]).astype(BF16)
            return halves(updated, upper_of(rtile_s[at, :]))

        joined = [None] * subs
        added = [None] * subs
        joined[0] = gathered(0)
        for c in range(1, subs + 1):
            if c < subs:
                joined[c] = gathered(c)
            added[c - 1] = middle(c - 1, joined[c - 1])
            joined[c - 1] = None
        group = 4
        for g in range(0, subs, group):
            row = rrow[:, g * sub : (g + group) * sub] % rhalf
            agg_s[...] += dot(rows_match(row, rhalf), jnp.concatenate(added[g : g + group], axis=0))
        return carry

    lax.fori_loop(0, turns, forward, 0)
    load_ncot.wait()
    latent = lat_ref[...]
    w_node = nin_ref[:width, :]
    w_agg = nin_ref[width:, :]
    cot = ncot_s[...].astype(F32)
    agg = jnp.concatenate([agg_s[:, :width], agg_s[:, width:]], axis=0).astype(BF16)
    node_pre = dot(jnp.concatenate([latent, agg], axis=1), nin_ref[...])
    sigma = sigmoid(node_pre)
    hidden = node_pre * sigma
    node_mid = dot(hidden.astype(BF16), nout_ref[...])
    grad_mid = norm_back(node_mid, ngain_ref[...], cot).astype(BF16)
    grad_pre = (
        dot_t(grad_mid, nout_ref[...]) * (sigma + hidden * (1.0 - sigma))
    ).astype(BF16)
    gagg = dot_t(grad_pre, w_agg).astype(BF16)
    gtab_s[...] = jnp.concatenate([gagg[:rhalf], gagg[rhalf:]], axis=1)
    gnode_s[...] = cot + dot_t(grad_pre, w_node)

    sub = 512
    subs = block // sub
    holder = lax.broadcasted_iota(jnp.int32, (sub, LANES), 1) // 8
    holder = holder.astype(F32).astype(BF16)

    def backward(t, carry):
        ecot_copy(t).wait()

        def place_of(c):
            return pl.ds(pl.multiple_of(t * block + c * sub, sub), sub)

        def gathered(c):
            at = place_of(c)
            upper = upper_of(rtile_s[at, :])
            spread = picked(dot(tiles_match(rkey_s[at, :], rhalf // LANES), gtab_s[...]), upper)
            return ecot_s[at, :].astype(F32) + spread.astype(F32)

        def middle(c, grad_upd):
            at = place_of(c)
            normed = normed_s[at, :]
            scaled = grad_upd * egain_ref[...]
            inner = (
                scaled
                - jnp.mean(scaled, axis=-1, keepdims=True)
                - normed * jnp.mean(scaled * normed, axis=-1, keepdims=True)
            )
            grad_pre = paired(inner.astype(BF16), woutt_s[...]) * slope_s[at, :]
            hidden = grad_pre.astype(BF16)
            ghid_s[at, :] = hidden
            gedge_s[at, :] = grad_upd
            moved = (paired(hidden, wgeo_s[...]) * unit_s[at, :].astype(F32)).astype(BF16)
            zero = jnp.zeros_like(moved)
            return (
                jnp.where(holder == stile_s[at, :], moved, zero),
                jnp.where(holder == rtile_s[at, :], moved, zero),
            )

        upd = [None] * subs
        pairs = [None] * subs
        upd[0] = gathered(0)
        for c in range(1, subs + 1):
            if c < subs:
                upd[c] = gathered(c)
            pairs[c - 1] = middle(c - 1, upd[c - 1])
            upd[c - 1] = None
        srow = compact_row(sidx_ref[t], nodes, slots)
        rrow = ridx_ref[t]
        sgeo_s[...] += dot(
            rows_match(srow % LANES, LANES), jnp.concatenate([p[0] for p in pairs], axis=0)
        )
        rgeo_s[...] += dot(
            rows_match(rrow % LANES, LANES), jnp.concatenate([p[1] for p in pairs], axis=0)
        )
        return carry

    lax.fori_loop(0, turns, backward, 0)
    sgeo = jnp.transpose(sgeo_s[...])
    rgeo = jnp.transpose(rgeo_s[...])
    tiles = []
    for t in range(every // LANES):
        tile = sgeo[8 * t : 8 * t + 8]
        if t < nodes // LANES:
            tile = tile - rgeo[8 * t : 8 * t + 8]
        tiles.append(tile + pltpu.roll(tile, 4, 0))
    gpos = jnp.concatenate(tiles, axis=1)
    gpos = jnp.where(lax.broadcasted_iota(jnp.int32, gpos.shape, 0) < 3, gpos, 0.0)
    hi = gpos.astype(BF16).astype(F32)
    both = jnp.concatenate([hi, gpos - hi], axis=0).astype(BF16)
    amp = dot(both, phi_s[...])
    amp = amp[0:8] + amp[8:16]
    for j in range(ctrl_ref.shape[0]):
        ctrl_ref[j] = amp[0:4, j * LANES : (j + 1) * LANES]
    sum_s[...] = jnp.zeros_like(sum_s)
    for k, (inside, _) in enumerate(partners):

        @pl.when(jnp.logical_not(inside))
        def _():
            got_s[k] = jnp.zeros_like(got_s[k])

    chunks = ctrl_ref.shape[0]
    reducers = max(r for r in range(1, parts + 1) if chunks % r == 0)
    per = chunks // reducers
    def part_copy(i):
        other = others[i]
        return remote(
            ctrl_ref.at[pl.ds(jnp.minimum(other, reducers - 1) * per, per)],
            part_s.at[i],
            part_send.at[i],
            part_recv.at[i],
            other,
        )

    def all_copy(i):
        return remote(
            mine_s,
            all_s.at[pl.ds(jnp.minimum(me, reducers - 1) * per, per)],
            all_send.at[i],
            all_recv.at[i],
            others[i],
        )

    def when_reducer(device, run):
        if reducers == parts:
            run()
        else:
            pl.when(device < reducers)(run)

    def sender_step(t, carry):
        srow = compact_row(sidx_ref[t], nodes, slots)
        stile = as_columns(srow // LANES)
        second = stile >= jnp.full_like(stile, shalf // LANES)
        values = ghid_s[pl.ds(pl.multiple_of(t * block, block), block), :]
        sum_s[...] += dot(rows_match(srow % shalf, shalf), halves(values, second))
        return carry

    for i in range(parts - 1):
        when_reducer(others[i], lambda: part_copy(i).start())
    lax.fori_loop(0, turns, sender_step, 0)
    back = dot(
        jnp.concatenate(split(sum_s[shalf - NEAR * slots :, width:]), axis=1),
        wnode_s[: 2 * width],
    ).astype(BF16)
    for k in range(NEAR):
        back_s[k] = back[k * slots : (k + 1) * slots]

    def back_copy(k):
        there = NEAR - 1 - k
        return remote(
            back_s.at[k], got_s.at[there], back_send.at[k], back_recv.at[there], partners[k][1]
        )

    def reduce_mine():
        total = ctrl_ref[pl.ds(jnp.minimum(me, reducers - 1) * per, per)]
        for i in range(parts - 1):
            part_copy(i).wait_recv()
        for i in range(parts - 1):
            total = total + part_s[i]
        mine_s[...] = total
        all_s[pl.ds(jnp.minimum(me, reducers - 1) * per, per)] = total

    def edge_step(t, carry):
        at = rows_of(t)
        gedge_s[at, :] = gedge_s[at, :] + paired(ghid_s[at, :], wedge_s[...])
        return carry

    lax.fori_loop(0, turns, edge_step, 0)
    for k, (inside, _) in enumerate(partners):

        @pl.when(inside)
        def _():
            back_copy(k).start()

    when_reducer(me, reduce_mine)
    rsum_s[...] = jnp.zeros_like(rsum_s)

    def send_all():
        for i in range(parts - 1):
            all_copy(i).start()

    when_reducer(me, send_all)

    def receiver_step(t, carry):
        rrow = ridx_ref[t]
        rtile = as_columns(rrow // LANES)
        upper = rtile >= jnp.full_like(rtile, rhalf // LANES)
        values = ghid_s[pl.ds(pl.multiple_of(t * block, block), block), :]
        rsum_s[...] += dot(rows_match(rrow % rhalf, rhalf), halves(values, upper))
        return carry

    lax.fori_loop(0, turns, receiver_step, 0)
    sent = jnp.concatenate([sum_s[:, :width], sum_s[: nodes - shalf, width:]], axis=0)
    received = jnp.concatenate([rsum_s[:, :width], rsum_s[:, width:]], axis=0)
    total = gnode_s[...] + dot(
        jnp.concatenate(split(sent) + split(received), axis=1), wnode_s[...]
    )
    for k, (inside, _) in enumerate(partners):

        @pl.when(inside)
        def _():
            back_copy(NEAR - 1 - k).wait_recv()

    rows = jnp.concatenate([rows_ref[0, pl.ds(partner, 1), :] for _, partner in partners], axis=1)
    got = jnp.concatenate([got_s[k] for k in range(NEAR)], axis=0)
    out_ref[...] = total + dot(rows_match(rows, nodes), got)
    for k, (inside, _) in enumerate(partners):

        @pl.when(inside)
        def _():
            back_copy(k).wait_send()

    for i in range(parts - 1):
        when_reducer(others[i], lambda: part_copy(i).wait_send())
    when_reducer(me, lambda: [all_copy(i).wait_send() for i in range(parts - 1)] and None)
    for i in range(parts - 1):
        source = sources[i]

        def arrived():
            remote(
                mine_s,
                all_s.at[pl.ds(jnp.minimum(source, reducers - 1) * per, per)],
                all_send.at[i],
                all_recv.at[i],
                others[i],
            ).wait_recv()

        when_reducer(source, arrived)
    for j in range(chunks):
        amp_out[:, j * LANES : (j + 1) * LANES] = all_s[j][0:3]


    for k, (inside, _) in enumerate(partners):

        @pl.when(inside)
        def _():
            for copy in copies(k):
                copy.wait_send()


def layer(args, parts):
    (lat, pos, cen, amp, rows, sidx, ridx, *weights, elat, ecot, ncot) = args
    nodes, width = lat.shape
    slots = rows.shape[2]
    controls = cen.shape[1]
    every = nodes + NEAR * slots
    turns, _, block = sidx.shape
    count = turns * block
    chunks = (controls // LANES, 4, LANES)
    reducers = max(r for r in range(1, parts + 1) if chunks[0] % r == 0)
    per = (chunks[0] // reducers,) + chunks[1:]
    like = lambda x: pltpu.VMEM(x.shape, x.dtype)
    dma = lambda n: pltpu.SemaphoreType.DMA((n,))
    edge = lambda kind: pltpu.VMEM((count, width), kind)
    small = [lat, pos, cen, amp, rows, sidx, ridx, *weights]
    return pl.pallas_call(
        functools.partial(layer_kernel, parts),
        in_specs=[pl.BlockSpec(memory_space=pltpu.HBM)] * len(args),
        out_specs=[VMEM_FULL] * 3,
        out_shape=[
            jax.ShapeDtypeStruct((count, width), F32),
            jax.ShapeDtypeStruct((nodes, width), F32),
            jax.ShapeDtypeStruct((3, controls), F32),
        ],
        scratch_shapes=[like(x) for x in small]
        + [
            dma(len(small)),
            pltpu.VMEM((NEAR, slots, width), BF16),
            pltpu.VMEM((8, every), F32),
            pltpu.VMEM((NEAR, slots, width), BF16),
            pltpu.VMEM((NEAR, 8, slots), F32),
            pltpu.VMEM((NEAR, 8, slots), F32),
            pltpu.VMEM((8, nodes), F32),
            pltpu.VMEM((LANES, controls), BF16),
            pltpu.VMEM((every, controls), BF16),
            dma(NEAR),
            dma(NEAR),
            dma(NEAR),
            dma(NEAR),
            edge(BF16),
            edge(BF16),
            like(ncot),
            edge(BF16),
            pltpu.VMEM((nodes, width), F32),
            dma(turns),
            dma(turns),
            pltpu.SemaphoreType.DMA,
            pltpu.VMEM((every // 2, 2 * width), BF16),
            pltpu.VMEM((nodes // 2, 2 * width), BF16),
            pltpu.VMEM((nodes // 2, 2 * width), BF16),
            pltpu.VMEM((3 * width + LANES, width), BF16),
            pltpu.VMEM((2 * width, 2 * width), BF16),
            pltpu.VMEM((2 * width, 2 * width), BF16),
            pltpu.VMEM((2 * width, 2 * width), BF16),
            pltpu.VMEM((2 * width, 2 * width), BF16),
            edge(BF16),
            pltpu.VMEM((4 * width, width), BF16),
            edge(F32),
            edge(F32),
            edge(BF16),
            edge(BF16),
            edge(BF16),
            edge(BF16),
            pltpu.VMEM((nodes // 2, 2 * width), F32),
            pltpu.VMEM((LANES, LANES), F32),
            pltpu.VMEM((LANES, LANES), F32),
            pltpu.VMEM(chunks, F32),
            pltpu.VMEM((every // 2, 2 * width), F32),
            pltpu.VMEM((nodes // 2, 2 * width), F32),
            pltpu.VMEM((NEAR, slots, width), BF16),
            pltpu.VMEM((NEAR, slots, width), BF16),
            pltpu.VMEM((parts - 1,) + per, F32),
            pltpu.VMEM(per, F32),
            pltpu.VMEM(chunks, F32),
            dma(NEAR),
            dma(NEAR),
            dma(parts - 1),
            dma(parts - 1),
            dma(parts - 1),
            dma(parts - 1),
        ],
        compiler_params=pltpu.CompilerParams(
            collective_id=0, has_side_effects=True, vmem_limit_bytes=46 * 1024 * 1024
        ),
        name="layer",
    )(*[pltpu.with_memory_space_constraint(x, pltpu.HBM) for x in args])


def leave_kernel(*refs):
    count = (len(refs) - 1) // 2
    copies = copy_all(list(zip(refs[:count], refs[count:-1])), refs[-1])
    for copy in copies:
        copy.wait()


def leave(*values):
    return pl.pallas_call(
        leave_kernel,
        in_specs=[VMEM_FULL] * len(values),
        out_specs=[ANY] * len(values),
        out_shape=[jax.ShapeDtypeStruct(x.shape, x.dtype) for x in values],
        scratch_shapes=[pltpu.SemaphoreType.DMA((len(values),))],
        compiler_params=pltpu.CompilerParams(vmem_limit_bytes=16 * 1024 * 1024),
        name="leave",
    )(*values)


def shards(
    node_latent,
    edge_latent,
    node_cot,
    edge_cot,
    base_pos,
    centers,
    amplitudes,
    edge_in,
    edge_geo,
    edge_out,
    edge_gain,
    node_in,
    node_out,
    node_gain,
    senders,
    receivers,
    send_rows,
):
    count = senders.shape[0]
    block = 1024 if count % 1024 == 0 else 512
    grad_edges, grad_nodes, grad_controls = leave(
        *layer(
            (
                node_latent,
                base_pos,
                centers,
                amplitudes,
                send_rows,
                senders.reshape(count // block, 1, block),
                receivers.reshape(count // block, 1, block),
                edge_in,
                edge_geo,
                edge_out,
                edge_gain[None, :],
                node_in,
                node_out,
                node_gain[None, :],
                edge_latent,
                edge_cot,
                node_cot,
            ),
            lax.axis_size("dom"),
        )
    )
    return (grad_nodes, grad_edges, grad_controls)


def solution(mesh):
    split_rows = P(("groups", "dom"), None)
    in_specs = (
        split_rows,
        split_rows,
        split_rows,
        split_rows,
        P(None, ("groups", "dom")),
        P(),
        P(),
        P(),
        P(),
        P(),
        P(),
        P(),
        P(),
        P(),
        P(("groups", "dom")),
        P(("groups", "dom")),
        P(("groups", "dom"), None, None),
    )
    out_specs = (split_rows, split_rows, P("groups", None))
    return jax.shard_map(shards, mesh=mesh, in_specs=in_specs, out_specs=out_specs, check_vma=False)
```

```python
import functools

import jax
import jax.numpy as jnp
from jax import lax
from jax.experimental import pallas as pl
from jax.experimental.pallas import tpu as pltpu
from jax.sharding import PartitionSpec as P

REACH = 2
RBF_RATE = 78.125
SCALE = (RBF_RATE * 1.4426950408889634) ** 0.5
FAR = 4.0 * SCALE
OFFSETS = [step for step in range(-REACH, REACH + 1) if step != 0]
NEAR = len(OFFSETS)
F32 = jnp.float32
BF16 = jnp.bfloat16
LANES = 128
VMEM_FULL = pl.BlockSpec(memory_space=pltpu.VMEM)
ANY = pl.BlockSpec(memory_space=pl.ANY)


def dot(a, b):
    return jnp.dot(a, b, preferred_element_type=F32)


def dot_t(a, b):
    return lax.dot_general(a, b, (((1,), (1,)), ((), ())), preferred_element_type=F32)


def stack_rows(rows, height):
    at = lax.broadcasted_iota(jnp.int32, (height, rows[0].shape[1]), 0)
    out = jnp.zeros(at.shape, F32)
    for k, row in enumerate(rows):
        if row is not None:
            out = jnp.where(at == k, row, out)
    return out


def split(x):
    hi = x.astype(BF16)
    return hi, (x - hi.astype(F32)).astype(BF16)


def three(x):
    hi = x.astype(BF16).astype(F32)
    rest = x - hi
    mid = rest.astype(BF16).astype(F32)
    return hi, mid, rest - mid


def as_columns(row):
    wide = jnp.broadcast_to(row.astype(F32), (LANES, row.shape[1])).astype(BF16)
    return jnp.transpose(wide)


def lane_iota(shape):
    return lax.broadcasted_iota(jnp.int32, shape, 1).astype(F32).astype(BF16)


def tiles_match(key, count):
    one, zero = jnp.ones_like(key), jnp.zeros_like(key)
    return jnp.concatenate(
        [jnp.where(key == jnp.full_like(key, j), one, zero) for j in range(count)], axis=1
    )


def columns_match(row, width):
    within = as_columns(row % LANES)
    tile = as_columns(row // LANES)
    key = jnp.where(within == lane_iota(within.shape), tile, jnp.full_like(tile, -1.0))
    return tiles_match(key, width // LANES)


def rows_match(row, height):
    block = row.shape[1]
    group = row // 16
    at = lax.broadcasted_iota(jnp.int32, (16, block), 0)
    key = jnp.where(at == row - group * 16, group, -1).astype(F32).astype(BF16)
    one, zero = jnp.ones_like(key), jnp.zeros_like(key)
    return jnp.concatenate(
        [jnp.where(key == jnp.full_like(key, q), one, zero) for q in range(height // 16)], axis=0
    )


def lane_gather(table_ref, row, count):
    block = row.shape[1]
    lane = jnp.broadcast_to(row % LANES, (8, block))
    tile = jnp.broadcast_to(row // LANES, (8, block))
    pieces = []
    for j in range(block // LANES):
        here = slice(j * LANES, (j + 1) * LANES)
        out = jnp.zeros((8, LANES), F32)
        for c in range(count):
            source = table_ref[:, c * LANES : (c + 1) * LANES]
            taken = jnp.take_along_axis(source, lane[:, here], axis=1, mode="promise_in_bounds")
            out = jnp.where(tile[:, here] == c, taken, out)
        pieces.append(out)
    return jnp.concatenate(pieces, axis=1)


def compact_row(raw, nodes, slots):
    me = lax.axis_index("dom")
    slot = jnp.maximum(raw - nodes, 0)
    off = slot // slots - me
    near = jnp.clip(jnp.where(off < 0, off + REACH, off + REACH - 1), 0, NEAR - 1)
    return jnp.where(raw >= nodes, nodes + near * slots + slot % slots, raw)


def neighbours(parts):
    me = lax.axis_index("dom")
    out = []
    for off in OFFSETS:
        there = me + off
        inside = (there >= 0) & (there < parts)
        out.append((inside, lax.rem(there + parts, parts)))
    return out


def remote(src, dst, send_sem, recv_sem, partner):
    return pltpu.make_async_remote_copy(
        src_ref=src,
        dst_ref=dst,
        send_sem=send_sem,
        recv_sem=recv_sem,
        device_id={"dom": partner},
        device_id_type=pl.DeviceIdType.MESH,
    )


def copy_all(pairs, sems):
    copies = [
        pltpu.make_async_copy(source, target, sems.at[i]) for i, (source, target) in enumerate(pairs)
    ]
    for copy in copies:
        copy.start()
    return copies


def normed_of(values):
    centred = values - jnp.mean(values, axis=-1, keepdims=True)
    inv = lax.rsqrt(jnp.mean(centred * centred, axis=-1, keepdims=True) + 1e-05)
    return centred * inv, inv


def norm_back(values, gain, upstream):
    normed, inv = normed_of(values)
    scaled = upstream * gain
    return inv * (
        scaled
        - jnp.mean(scaled, axis=-1, keepdims=True)
        - normed * jnp.mean(scaled * normed, axis=-1, keepdims=True)
    )


def sigmoid(values):
    return 0.5 * jnp.tanh(0.5 * values) + 0.5


def paired(values, weights):
    half = values.shape[0] // 2
    out = dot(jnp.concatenate([values[:half], values[half:]], axis=1), weights)
    return jnp.concatenate([out[:, :LANES], out[:, LANES:]], axis=0)


def picked(pair, second):
    pair = pair.astype(BF16)
    return jnp.where(second, pair[:, LANES:], pair[:, :LANES])


def halves(values, second):
    zero = jnp.zeros_like(values)
    return jnp.concatenate([jnp.where(second, zero, values), jnp.where(second, values, zero)], axis=1)


def layer_kernel(parts, *refs):
    (
        lat_hbm,
        pos_hbm,
        cen_hbm,
        amp_hbm,
        rows_hbm,
        sidx_hbm,
        ridx_hbm,
        ein_hbm,
        egeo_hbm,
        eout_hbm,
        egain_hbm,
        nin_hbm,
        nout_hbm,
        ngain_hbm,
        elat_hbm,
        ecot_hbm,
        ncot_hbm,
        gedge_s,
        out_ref,
        amp_out,
        lat_ref,
        pos_ref,
        cen_ref,
        amp_ref,
        rows_ref,
        sidx_ref,
        ridx_ref,
        ein_ref,
        egeo_ref,
        eout_ref,
        egain_ref,
        nin_ref,
        nout_ref,
        ngain_ref,
        load_sem,
        halo_ref,
        place_ref,
        out_s,
        pout_s,
        pin_s,
        base_s,
        cmat_s,
        phi_s,
        send_sem,
        recv_sem,
        psend_sem,
        precv_sem,
        elat_s,
        ecot_s,
        ncot_s,
        ghid_s,
        gnode_s,
        elat_sem,
        ecot_sem,
        ncot_sem,
        stab_s,
        rtab_s,
        gtab_s,
        win_s,
        wout_s,
        woutt_s,
        wgeo_s,
        wedge_s,
        peer_s,
        wnode_s,
        slope_s,
        normed_s,
        rkey_s,
        rtile_s,
        stile_s,
        unit_s,
        agg_s,
        sgeo_s,
        rgeo_s,
        ctrl_ref,
        sum_s,
        rsum_s,
        back_s,
        got_s,
        part_s,
        mine_s,
        all_s,
        back_send,
        back_recv,
        part_send,
        part_recv,
        all_send,
        all_recv,
    ) = refs
    nodes = lat_ref.shape[0]
    slots = rows_ref.shape[2]
    controls = cen_ref.shape[1]
    partners = neighbours(parts)
    me = lax.axis_index("dom")
    others = [lax.rem(me + i, parts) for i in range(1, parts)]
    sources = [lax.rem(me + parts - i, parts) for i in range(1, parts)]
    barrier = pltpu.get_barrier_semaphore()
    for other in others:
        pl.semaphore_signal(
            barrier, inc=1, device_id={"dom": other}, device_id_type=pl.DeviceIdType.MESH
        )
    loads = copy_all(
        [
            (rows_hbm, rows_ref),
            (lat_hbm, lat_ref),
            (pos_hbm, pos_ref),
            (cen_hbm, cen_ref),
            (amp_hbm, amp_ref),
            (sidx_hbm, sidx_ref),
            (ridx_hbm, ridx_ref),
            (ein_hbm, ein_ref),
            (egeo_hbm, egeo_ref),
            (eout_hbm, eout_ref),
            (egain_hbm, egain_ref),
            (nin_hbm, nin_ref),
            (nout_hbm, nout_ref),
            (ngain_hbm, ngain_ref),
        ],
        load_sem,
    )
    width = lat_ref.shape[1]
    away = NEAR * slots
    every = nodes + away
    turns, _, block = sidx_ref.shape
    shalf = every // 2
    rhalf = nodes // 2

    def rows_of(t):
        return pl.ds(pl.multiple_of(t * block, block), block)

    def elat_copy(t):
        return pltpu.make_async_copy(elat_hbm.at[rows_of(t)], elat_s.at[rows_of(t)], elat_sem.at[t])

    def ecot_copy(t):
        return pltpu.make_async_copy(ecot_hbm.at[rows_of(t)], ecot_s.at[rows_of(t)], ecot_sem.at[t])

    for t in range(turns):
        elat_copy(t).start()
    load_ncot = pltpu.make_async_copy(ncot_hbm, ncot_s, ncot_sem)
    load_ncot.start()
    for t in range(turns):
        ecot_copy(t).start()
    for load in loads[:5]:
        load.wait()
    rows = [rows_ref[0, pl.ds(partner, 1), :] for _, partner in partners]
    base_s[...] = stack_rows([pos_ref[k : k + 1, :] for k in range(3)], 8)
    match = columns_match(jnp.concatenate(rows, axis=1), nodes)
    taken = dot(match, lat_ref[...]).astype(BF16)
    for k in range(NEAR):
        out_s[k] = taken[k * slots : (k + 1) * slots]
        pout_s[k] = lane_gather(base_s, rows[k], nodes // LANES)
    for k, (inside, _) in enumerate(partners):

        @pl.when(jnp.logical_not(inside))
        def _():
            halo_ref[k] = jnp.zeros_like(halo_ref[k])
            pin_s[k] = jnp.zeros_like(pin_s[k])

    def copies(k):
        there = NEAR - 1 - k
        partner = partners[k][1]
        return (
            remote(out_s.at[k], halo_ref.at[there], send_sem.at[k], recv_sem.at[there], partner),
            remote(pout_s.at[k], pin_s.at[there], psend_sem.at[k], precv_sem.at[there], partner),
        )

    cen = [SCALE * (cen_ref[k : k + 1, :] - 0.5) for k in range(3)]
    crows = []
    for k in range(3):
        hi, mid, low = three(cen[k])
        crows += [hi, mid, hi, low, mid, hi]
    ones = jnp.ones_like(cen[0])
    crows += [ones, ones, ones]
    crows += list(three(-(cen[0] * cen[0] + cen[1] * cen[1] + cen[2] * cen[2])))
    cmat_s[...] = jnp.concatenate(
        [stack_rows(crows[j : j + 8], 8) for j in range(0, 24, 8)]
        + [jnp.zeros((LANES - 24, controls), F32)],
        axis=0,
    ).astype(BF16)
    amp = stack_rows([amp_ref[k : k + 1, :] for k in range(3)], 8)
    amp_hi = amp.astype(BF16).astype(F32)
    amp16 = jnp.concatenate([amp_hi, amp - amp_hi], axis=0).astype(BF16)

    def radial(base, first, size, index=0):
        moved = jnp.clip(SCALE * (base - 0.5), -FAR, FAR)
        parts_of = [three(moved[k : k + 1]) for k in range(3)]
        prows = []
        for hi, mid, low in parts_of:
            hi2, mid2, low2 = 2.0 * hi, 2.0 * mid, 2.0 * low
            prows += [hi2, hi2, mid2, hi2, mid2, low2]
        norm = moved[0:1] * moved[0:1] + moved[1:2] * moved[1:2] + moved[2:3] * moved[2:3]
        prows += list(three(-norm))
        one = jnp.ones_like(norm)
        prows += [one, one, one]
        wide = jnp.concatenate(
            [stack_rows(prows[j : j + 8], 8) for j in range(0, 24, 8)]
            + [jnp.zeros((LANES - 24, size), F32)],
            axis=0,
        )
        left = jnp.transpose(wide).astype(BF16)
        phi = jnp.exp2(dot(left, cmat_s[...])).astype(BF16)
        phi_s[pl.ds(first, size), :] = phi
        shift = dot_t(amp16, phi)
        place_ref[:, pl.ds(first, size)] = base + (shift[0:8] + shift[8:16])

    size = 256
    own = nodes // size

    def own_step(i, carry):
        first = pl.multiple_of(i * size, size)
        radial(base_s[:, pl.ds(first, size)], first, size, i)
        return carry

    lax.fori_loop(0, own, own_step, 0)
    pl.semaphore_wait(barrier, parts - 1)

    for k, (inside, _) in enumerate(partners):

        @pl.when(inside)
        def _():
            for copy in copies(k):
                copy.start()

    for load in loads[5:]:
        load.wait()
    agg_s[...] = jnp.zeros_like(agg_s)
    sgeo_s[...] = jnp.zeros_like(sgeo_s)
    rgeo_s[...] = jnp.zeros_like(rgeo_s)
    stab_s[:, :width] = lat_ref[:shalf]
    stab_s[: nodes - shalf, width:] = lat_ref[shalf:]
    rtab_s[:, :width] = lat_ref[:rhalf]
    rtab_s[:, width:] = lat_ref[rhalf:]
    geo = stack_rows([egeo_ref[k : k + 1, :] for k in range(4)], 8)
    hi = geo.astype(BF16).astype(F32)
    win_s[: 3 * width] = ein_ref[...]
    win_s[3 * width :] = jnp.concatenate(
        [hi + pltpu.roll(hi, 4, 0), geo - hi, jnp.zeros((LANES - 16, width), F32)], axis=0
    ).astype(BF16)
    w_out = eout_ref[...]
    zero = jnp.zeros_like(w_out)
    turned = jnp.transpose(w_out.astype(F32)).astype(BF16)
    wout_s[...] = jnp.concatenate(
        [jnp.concatenate([w_out, zero], axis=1), jnp.concatenate([zero, w_out], axis=1)], axis=0
    )
    woutt_s[...] = jnp.concatenate(
        [jnp.concatenate([turned, zero], axis=1), jnp.concatenate([zero, turned], axis=1)],
        axis=0,
    )
    w_edge = jnp.transpose(ein_ref[2 * width :].astype(F32)).astype(BF16)
    third = egeo_ref[3:4, :]
    spread = stack_rows(
        [egeo_ref[k : k + 1, :] for k in range(3)] + [None, third, third, third], 8
    )
    spread = jnp.transpose(jnp.concatenate([spread] * (LANES // 8), axis=0)).astype(BF16)
    w_send = jnp.transpose(ein_ref[:width].astype(F32)).astype(BF16)
    w_recv = jnp.transpose(ein_ref[width : 2 * width].astype(F32)).astype(BF16)
    wnode_s[...] = jnp.concatenate([w_send, w_send, w_recv, w_recv], axis=0)
    wgeo_s[...] = jnp.concatenate(
        [jnp.concatenate([spread, zero], axis=1), jnp.concatenate([zero, spread], axis=1)], axis=0
    )
    wedge_s[...] = jnp.concatenate(
        [jnp.concatenate([w_edge, zero], axis=1), jnp.concatenate([zero, w_edge], axis=1)], axis=0
    )

    def upper_of(tile):
        return tile >= jnp.full_like(tile, rhalf // LANES)

    def receive(t, carry):
        at = rows_of(t)
        rrow = ridx_ref[t]
        rtile = as_columns(rrow // LANES)
        upper = upper_of(rtile)
        local = jnp.where(upper, rtile - jnp.full_like(rtile, rhalf // LANES), rtile)
        none = jnp.full_like(rtile, -1.0)
        rkey = jnp.where(as_columns(rrow % LANES) == lane_iota(rtile.shape), local, none)
        peer_s[at, :] = picked(dot(tiles_match(rkey, rhalf // LANES), rtab_s[...]), upper)
        rtile_s[at, :] = rtile
        rkey_s[at, :] = rkey
        return carry

    lax.fori_loop(0, turns, receive, 0)
    for k, (inside, _) in enumerate(partners):

        @pl.when(inside)
        def _():
            for copy in copies(NEAR - 1 - k):
                copy.wait_recv()

    pair = size // slots
    for j in range(NEAR // pair):
        halo = jnp.concatenate([pin_s[j * pair + i] for i in range(pair)], axis=1)
        radial(halo, nodes + j * size, size, own + j)
    for k in range(NEAR):
        stab_s[nodes - shalf + k * slots : nodes - shalf + (k + 1) * slots, width:] = halo_ref[k]

    sub = 256
    subs = block // sub

    def forward(t, carry):
        srow = compact_row(sidx_ref[t], nodes, slots)
        rrow = ridx_ref[t]
        elat_copy(t).wait()
        delta = lane_gather(place_ref, srow, every // LANES) - lane_gather(
            place_ref, rrow, nodes // LANES
        )
        length = jnp.sqrt(jnp.sum(delta * delta, axis=0, keepdims=True) + 0.01)
        level = lax.broadcasted_iota(jnp.int32, delta.shape, 0)
        geo = jnp.where(level == 3, length, delta)
        hi = geo.astype(BF16).astype(F32)
        wide = jnp.concatenate(
            [hi + pltpu.roll(geo - hi, 4, 0), hi, jnp.zeros((LANES - 16, block), F32)], axis=0
        ).astype(BF16)
        unit = jnp.where(level < 3, 1.0, pltpu.roll(delta * (1.0 / length), 4, 0)).astype(F32)
        unit = jnp.concatenate([unit] * (LANES // 8), axis=0).astype(BF16)
        lane = lane_iota((sub, LANES))
        none = jnp.full_like(lane, -1.0)

        def place_of(c):
            return pl.ds(pl.multiple_of(t * block + c * sub, sub), sub)

        def gathered(c):
            here = slice(c * sub, (c + 1) * sub)
            at = place_of(c)
            stile = as_columns(srow[:, here] // LANES)
            shift = jnp.full_like(stile, shalf // LANES)
            second = stile >= shift
            local = jnp.where(second, stile - shift, stile)
            skey = jnp.where(as_columns(srow[:, here] % LANES) == lane, local, none)
            sent = picked(dot(tiles_match(skey, shalf // LANES), stab_s[...]), second)
            stile_s[at, :] = stile
            unit_s[at, :] = jnp.transpose(unit[:, here])
            return jnp.concatenate(
                [sent, peer_s[at, :], elat_s[at, :], jnp.transpose(wide[:, here])], axis=1
            )

        def middle(c, joined):
            at = place_of(c)
            pre = dot(joined, win_s[...])
            sigma = sigmoid(pre)
            hidden = pre * sigma
            slope = sigma + hidden * (1.0 - sigma)
            normed, inv = normed_of(paired(hidden.astype(BF16), wout_s[...]))
            slope_s[at, :] = slope * inv
            normed_s[at, :] = normed
            latent = joined[:, 2 * width : 3 * width]
            updated = (latent.astype(F32) + normed * egain_ref[...]).astype(BF16)
            return halves(updated, upper_of(rtile_s[at, :]))

        joined = [None] * subs
        added = [None] * subs
        joined[0] = gathered(0)
        for c in range(1, subs + 1):
            if c < subs:
                joined[c] = gathered(c)
            added[c - 1] = middle(c - 1, joined[c - 1])
            joined[c - 1] = None
        group = subs
        for g in range(0, subs, group):
            row = rrow[:, g * sub : (g + group) * sub] % rhalf
            agg_s[...] += dot(rows_match(row, rhalf), jnp.concatenate(added[g : g + group], axis=0))
        return carry

    lax.fori_loop(0, turns, forward, 0)
    load_ncot.wait()
    latent = lat_ref[...]
    w_node = nin_ref[:width, :]
    w_agg = nin_ref[width:, :]
    cot = ncot_s[...].astype(F32)
    agg = jnp.concatenate([agg_s[:, :width], agg_s[:, width:]], axis=0).astype(BF16)
    node_pre = dot(jnp.concatenate([latent, agg], axis=1), nin_ref[...])
    sigma = sigmoid(node_pre)
    hidden = node_pre * sigma
    node_mid = dot(hidden.astype(BF16), nout_ref[...])
    grad_mid = norm_back(node_mid, ngain_ref[...], cot).astype(BF16)
    grad_pre = (
        dot_t(grad_mid, nout_ref[...]) * (sigma + hidden * (1.0 - sigma))
    ).astype(BF16)
    gagg = dot_t(grad_pre, w_agg).astype(BF16)
    gtab_s[...] = jnp.concatenate([gagg[:rhalf], gagg[rhalf:]], axis=1)
    gnode_s[...] = cot + dot_t(grad_pre, w_node)

    sub = 512
    subs = block // sub
    holder = lax.broadcasted_iota(jnp.int32, (sub, LANES), 1) // 8
    holder = holder.astype(F32).astype(BF16)

    def backward(t, carry):
        ecot_copy(t).wait()

        def place_of(c):
            return pl.ds(pl.multiple_of(t * block + c * sub, sub), sub)

        def gathered(c):
            at = place_of(c)
            upper = upper_of(rtile_s[at, :])
            spread = picked(dot(tiles_match(rkey_s[at, :], rhalf // LANES), gtab_s[...]), upper)
            return ecot_s[at, :].astype(F32) + spread.astype(F32)

        def middle(c, grad_upd):
            at = place_of(c)
            normed = normed_s[at, :]
            scaled = grad_upd * egain_ref[...]
            inner = (
                scaled
                - jnp.mean(scaled, axis=-1, keepdims=True)
                - normed * jnp.mean(scaled * normed, axis=-1, keepdims=True)
            )
            grad_pre = paired(inner.astype(BF16), woutt_s[...]) * slope_s[at, :]
            hidden = grad_pre.astype(BF16)
            ghid_s[at, :] = hidden
            gedge_s[at, :] = grad_upd
            moved = (paired(hidden, wgeo_s[...]) * unit_s[at, :].astype(F32)).astype(BF16)
            zero = jnp.zeros_like(moved)
            return (
                jnp.where(holder == stile_s[at, :], moved, zero),
                jnp.where(holder == rtile_s[at, :], moved, zero),
            )

        upd = [None] * subs
        pairs = [None] * subs
        upd[0] = gathered(0)
        for c in range(1, subs + 1):
            if c < subs:
                upd[c] = gathered(c)
            pairs[c - 1] = middle(c - 1, upd[c - 1])
            upd[c - 1] = None
        srow = compact_row(sidx_ref[t], nodes, slots)
        rrow = ridx_ref[t]
        sgeo_s[...] += dot(
            rows_match(srow % LANES, LANES), jnp.concatenate([p[0] for p in pairs], axis=0)
        )
        rgeo_s[...] += dot(
            rows_match(rrow % LANES, LANES), jnp.concatenate([p[1] for p in pairs], axis=0)
        )
        return carry

    lax.fori_loop(0, turns, backward, 0)
    sgeo = jnp.transpose(sgeo_s[...])
    rgeo = jnp.transpose(rgeo_s[...])
    tiles = []
    for t in range(every // LANES):
        tile = sgeo[8 * t : 8 * t + 8]
        if t < nodes // LANES:
            tile = tile - rgeo[8 * t : 8 * t + 8]
        tiles.append(tile + pltpu.roll(tile, 4, 0))
    gpos = jnp.concatenate(tiles, axis=1)
    gpos = jnp.where(lax.broadcasted_iota(jnp.int32, gpos.shape, 0) < 3, gpos, 0.0)
    hi = gpos.astype(BF16).astype(F32)
    both = jnp.concatenate([hi, gpos - hi], axis=0).astype(BF16)
    amp = dot(both, phi_s[...])
    amp = amp[0:8] + amp[8:16]
    for j in range(ctrl_ref.shape[0]):
        ctrl_ref[j] = amp[0:4, j * LANES : (j + 1) * LANES]
    sum_s[...] = jnp.zeros_like(sum_s)
    for k, (inside, _) in enumerate(partners):

        @pl.when(jnp.logical_not(inside))
        def _():
            got_s[k] = jnp.zeros_like(got_s[k])

    chunks = ctrl_ref.shape[0]
    reducers = max(r for r in range(1, parts + 1) if chunks % r == 0)
    per = chunks // reducers
    def part_copy(i):
        other = others[i]
        return remote(
            ctrl_ref.at[pl.ds(jnp.minimum(other, reducers - 1) * per, per)],
            part_s.at[i],
            part_send.at[i],
            part_recv.at[i],
            other,
        )

    def all_copy(i):
        return remote(
            mine_s,
            all_s.at[pl.ds(jnp.minimum(me, reducers - 1) * per, per)],
            all_send.at[i],
            all_recv.at[i],
            others[i],
        )

    def when_reducer(device, run):
        if reducers == parts:
            run()
        else:
            pl.when(device < reducers)(run)

    def sender_step(t, carry):
        srow = compact_row(sidx_ref[t], nodes, slots)
        stile = as_columns(srow // LANES)
        second = stile >= jnp.full_like(stile, shalf // LANES)
        values = ghid_s[pl.ds(pl.multiple_of(t * block, block), block), :]
        sum_s[...] += dot(rows_match(srow % shalf, shalf), halves(values, second))
        return carry

    for i in range(parts - 1):
        when_reducer(others[i], lambda: part_copy(i).start())
    lax.fori_loop(0, turns, sender_step, 0)
    back = dot(
        jnp.concatenate(split(sum_s[shalf - NEAR * slots :, width:]), axis=1),
        wnode_s[: 2 * width],
    ).astype(BF16)
    for k in range(NEAR):
        back_s[k] = back[k * slots : (k + 1) * slots]

    def back_copy(k):
        there = NEAR - 1 - k
        return remote(
            back_s.at[k], got_s.at[there], back_send.at[k], back_recv.at[there], partners[k][1]
        )

    def reduce_mine():
        total = ctrl_ref[pl.ds(jnp.minimum(me, reducers - 1) * per, per)]
        for i in range(parts - 1):
            part_copy(i).wait_recv()
        for i in range(parts - 1):
            total = total + part_s[i]
        mine_s[...] = total
        all_s[pl.ds(jnp.minimum(me, reducers - 1) * per, per)] = total

    def edge_step(t, carry):
        at = rows_of(t)
        gedge_s[at, :] = gedge_s[at, :] + paired(ghid_s[at, :], wedge_s[...])
        return carry

    lax.fori_loop(0, turns, edge_step, 0)
    for k, (inside, _) in enumerate(partners):

        @pl.when(inside)
        def _():
            back_copy(k).start()

    when_reducer(me, reduce_mine)
    rsum_s[...] = jnp.zeros_like(rsum_s)

    def send_all():
        for i in range(parts - 1):
            all_copy(i).start()

    when_reducer(me, send_all)

    def receiver_step(t, carry):
        rrow = ridx_ref[t]
        rtile = as_columns(rrow // LANES)
        upper = rtile >= jnp.full_like(rtile, rhalf // LANES)
        values = ghid_s[pl.ds(pl.multiple_of(t * block, block), block), :]
        rsum_s[...] += dot(rows_match(rrow % rhalf, rhalf), halves(values, upper))
        return carry

    lax.fori_loop(0, turns, receiver_step, 0)
    sent = jnp.concatenate([sum_s[:, :width], sum_s[: nodes - shalf, width:]], axis=0)
    received = jnp.concatenate([rsum_s[:, :width], rsum_s[:, width:]], axis=0)
    total = gnode_s[...] + dot(
        jnp.concatenate(split(sent) + split(received), axis=1), wnode_s[...]
    )
    for k, (inside, _) in enumerate(partners):

        @pl.when(inside)
        def _():
            back_copy(NEAR - 1 - k).wait_recv()

    rows = jnp.concatenate([rows_ref[0, pl.ds(partner, 1), :] for _, partner in partners], axis=1)
    got = jnp.concatenate([got_s[k] for k in range(NEAR)], axis=0)
    out_ref[...] = total + dot(rows_match(rows, nodes), got)
    for k, (inside, _) in enumerate(partners):

        @pl.when(inside)
        def _():
            back_copy(k).wait_send()

    for i in range(parts - 1):
        when_reducer(others[i], lambda: part_copy(i).wait_send())
    when_reducer(me, lambda: [all_copy(i).wait_send() for i in range(parts - 1)] and None)
    for i in range(parts - 1):
        source = sources[i]

        def arrived():
            remote(
                mine_s,
                all_s.at[pl.ds(jnp.minimum(source, reducers - 1) * per, per)],
                all_send.at[i],
                all_recv.at[i],
                others[i],
            ).wait_recv()

        when_reducer(source, arrived)
    for j in range(chunks):
        amp_out[:, j * LANES : (j + 1) * LANES] = all_s[j][0:3]


    for k, (inside, _) in enumerate(partners):

        @pl.when(inside)
        def _():
            for copy in copies(k):
                copy.wait_send()


def layer(args, parts):
    (lat, pos, cen, amp, rows, sidx, ridx, *weights, elat, ecot, ncot) = args
    nodes, width = lat.shape
    slots = rows.shape[2]
    controls = cen.shape[1]
    every = nodes + NEAR * slots
    turns, _, block = sidx.shape
    count = turns * block
    chunks = (controls // LANES, 4, LANES)
    reducers = max(r for r in range(1, parts + 1) if chunks[0] % r == 0)
    per = (chunks[0] // reducers,) + chunks[1:]
    like = lambda x: pltpu.VMEM(x.shape, x.dtype)
    dma = lambda n: pltpu.SemaphoreType.DMA((n,))
    edge = lambda kind: pltpu.VMEM((count, width), kind)
    small = [lat, pos, cen, amp, rows, sidx, ridx, *weights]
    return pl.pallas_call(
        functools.partial(layer_kernel, parts),
        in_specs=[pl.BlockSpec(memory_space=pltpu.HBM)] * len(args),
        out_specs=[VMEM_FULL] * 3,
        out_shape=[
            jax.ShapeDtypeStruct((count, width), F32),
            jax.ShapeDtypeStruct((nodes, width), F32),
            jax.ShapeDtypeStruct((3, controls), F32),
        ],
        scratch_shapes=[like(x) for x in small]
        + [
            dma(len(small)),
            pltpu.VMEM((NEAR, slots, width), BF16),
            pltpu.VMEM((8, every), F32),
            pltpu.VMEM((NEAR, slots, width), BF16),
            pltpu.VMEM((NEAR, 8, slots), F32),
            pltpu.VMEM((NEAR, 8, slots), F32),
            pltpu.VMEM((8, nodes), F32),
            pltpu.VMEM((LANES, controls), BF16),
            pltpu.VMEM((every, controls), BF16),
            dma(NEAR),
            dma(NEAR),
            dma(NEAR),
            dma(NEAR),
            edge(BF16),
            edge(BF16),
            like(ncot),
            edge(BF16),
            pltpu.VMEM((nodes, width), F32),
            dma(turns),
            dma(turns),
            pltpu.SemaphoreType.DMA,
            pltpu.VMEM((every // 2, 2 * width), BF16),
            pltpu.VMEM((nodes // 2, 2 * width), BF16),
            pltpu.VMEM((nodes // 2, 2 * width), BF16),
            pltpu.VMEM((3 * width + LANES, width), BF16),
            pltpu.VMEM((2 * width, 2 * width), BF16),
            pltpu.VMEM((2 * width, 2 * width), BF16),
            pltpu.VMEM((2 * width, 2 * width), BF16),
            pltpu.VMEM((2 * width, 2 * width), BF16),
            edge(BF16),
            pltpu.VMEM((4 * width, width), BF16),
            edge(F32),
            edge(F32),
            edge(BF16),
            edge(BF16),
            edge(BF16),
            edge(BF16),
            pltpu.VMEM((nodes // 2, 2 * width), F32),
            pltpu.VMEM((LANES, LANES), F32),
            pltpu.VMEM((LANES, LANES), F32),
            pltpu.VMEM(chunks, F32),
            pltpu.VMEM((every // 2, 2 * width), F32),
            pltpu.VMEM((nodes // 2, 2 * width), F32),
            pltpu.VMEM((NEAR, slots, width), BF16),
            pltpu.VMEM((NEAR, slots, width), BF16),
            pltpu.VMEM((parts - 1,) + per, F32),
            pltpu.VMEM(per, F32),
            pltpu.VMEM(chunks, F32),
            dma(NEAR),
            dma(NEAR),
            dma(parts - 1),
            dma(parts - 1),
            dma(parts - 1),
            dma(parts - 1),
        ],
        compiler_params=pltpu.CompilerParams(
            collective_id=0, has_side_effects=True, vmem_limit_bytes=46 * 1024 * 1024
        ),
        name="layer",
    )(*[pltpu.with_memory_space_constraint(x, pltpu.HBM) for x in args])


def leave_kernel(*refs):
    count = (len(refs) - 1) // 2
    copies = copy_all(list(zip(refs[:count], refs[count:-1])), refs[-1])
    for copy in copies:
        copy.wait()


def leave(*values):
    return pl.pallas_call(
        leave_kernel,
        in_specs=[VMEM_FULL] * len(values),
        out_specs=[ANY] * len(values),
        out_shape=[jax.ShapeDtypeStruct(x.shape, x.dtype) for x in values],
        scratch_shapes=[pltpu.SemaphoreType.DMA((len(values),))],
        compiler_params=pltpu.CompilerParams(vmem_limit_bytes=16 * 1024 * 1024),
        name="leave",
    )(*values)


def shards(
    node_latent,
    edge_latent,
    node_cot,
    edge_cot,
    base_pos,
    centers,
    amplitudes,
    edge_in,
    edge_geo,
    edge_out,
    edge_gain,
    node_in,
    node_out,
    node_gain,
    senders,
    receivers,
    send_rows,
):
    count = senders.shape[0]
    block = 2048 if count % 2048 == 0 else 512
    grad_edges, grad_nodes, grad_controls = leave(
        *layer(
            (
                node_latent,
                base_pos,
                centers,
                amplitudes,
                send_rows,
                senders.reshape(count // block, 1, block),
                receivers.reshape(count // block, 1, block),
                edge_in,
                edge_geo,
                edge_out,
                edge_gain[None, :],
                node_in,
                node_out,
                node_gain[None, :],
                edge_latent,
                edge_cot,
                node_cot,
            ),
            lax.axis_size("dom"),
        )
    )
    return (grad_nodes, grad_edges, grad_controls)


def solution(mesh):
    split_rows = P(("groups", "dom"), None)
    in_specs = (
        split_rows,
        split_rows,
        split_rows,
        split_rows,
        P(None, ("groups", "dom")),
        P(),
        P(),
        P(),
        P(),
        P(),
        P(),
        P(),
        P(),
        P(),
        P(("groups", "dom")),
        P(("groups", "dom")),
        P(("groups", "dom"), None, None),
    )
    out_specs = (split_rows, split_rows, P("groups", None))
    return jax.shard_map(shards, mesh=mesh, in_specs=in_specs, out_specs=out_specs, check_vma=False)
```
